128 devices in a mesh: blk: 2 (over core), dp: 64 (over z, y, x).
Axes of the slice: x: 4, y: 4, z: 4, core: 2. Of those that a mesh axis runs over, the one named last changes fastest.
Arguments:
- queries: bfloat16 [16384, 256], P(('blk', 'dp')), may hold values from -1 to 1, as said below
- items: bfloat16 [16384, 256], P(('blk', 'dp')), may hold values from -1 to 1, as said below
Outputs:
- loss: float32 [], replicated
- question_slope: float32 [16384, 256], P(('blk', 'dp'))
- candidate_slope: float32 [16384, 256], P(('blk', 'dp'))
The draws below stay inside these ranges and needn't reach their ends.
Inputs may be any that keep to these rules, and one draw needn't show every extreme that they name: queries: entries lie between -1 and 1 and no row is zero; each query is close to its own item and to one item of the batch chosen by a random permutation (which may be its own). items: entries lie between -1 and 1 and no row is zero.
All inputs are finite; a program needn't handle non-finite values.
Results may differ from the reference program's by a relative error of at most 0.008.
Values may be sent and summed in bfloat16 or wider, within the bound.
A program may use at most 64 MiB of HBM per device.

```python
import jax
import jax.numpy as jnp
from jax import lax

ROWS = 128
D = 256
BATCH = 16384


def pair_draw(key):
    items_raw = jax.random.truncated_normal(jax.random.fold_in(key, 11), -4.0, 4.0, (BATCH, D), jnp.float32) * 0.0625
    partner = jax.random.permutation(jax.random.fold_in(key, 12), BATCH)
    noise_part = jax.random.truncated_normal(jax.random.fold_in(key, 13), -4.0, 4.0, (BATCH, D), jnp.float32) * 0.0625
    mixture = 0.6 * items_raw + 0.6 * items_raw[partner] + 0.7 * noise_part
    return (mixture, items_raw)


def draw_queries(key, part):
    return pair_draw(key)[0].astype(jnp.bfloat16)


def draw_items(key, part):
    return pair_draw(key)[1].astype(jnp.bfloat16)


def setup_inputs(seed: int = 0) -> dict:
    seeds = jax.random.split(jax.random.key(seed), 3)
    queries = draw_queries(jax.random.fold_in(seeds[2], 71), 0)
    items = draw_items(jax.random.fold_in(seeds[2], 71), 0)
    return dict(queries=queries, items=items)


softmax_sharpness = 0.05
tiny_square = 1e-12

def unit_rows(matrix):
    widened = matrix.astype(jnp.float32)
    length = jnp.sqrt(lax.optimization_barrier(jnp.sum(widened * widened, axis=1, keepdims=True)) + tiny_square)
    return (widened / length, length)

def round_wide(values):
    return lax.optimization_barrier(values.astype(jnp.bfloat16)).astype(jnp.float32)

def direction_slope(grad, unit, length):
    along = lax.optimization_barrier(jnp.sum(unit * grad, axis=1, keepdims=True))
    return (grad - unit * along) / length

def reference(queries, items):
    question_direction, question_magnitude = unit_rows(queries)
    candidate_direction, candidate_magnitude = unit_rows(items)
    question_gathered_all = round_wide(question_direction)
    candidate_gathered_all = round_wide(candidate_direction)
    matching_score = lax.optimization_barrier(jnp.sum(question_gathered_all * candidate_gathered_all, axis=1)) / softmax_sharpness
    q_blocks = question_gathered_all.reshape(BATCH // ROWS, ROWS, D)

    def per_block(candidate_count_overall, question_portion):
        similarity_scores = jnp.dot(question_portion, candidate_gathered_all.T, precision=lax.Precision.HIGHEST) / softmax_sharpness
        new_peak = lax.optimization_barrier(jnp.max(similarity_scores, axis=1))
        log_norm = new_peak + jnp.log(lax.optimization_barrier(jnp.sum(jnp.exp(similarity_scores - new_peak[:, None]), axis=1)))
        weights = round_wide(jnp.exp(similarity_scores - log_norm[:, None]))
        question_count_overall = jnp.dot(weights, candidate_gathered_all, precision=lax.Precision.HIGHEST)
        candidate_count_overall = candidate_count_overall + jnp.dot(weights.T, question_portion, precision=lax.Precision.HIGHEST)
        return (candidate_count_overall, (log_norm, question_count_overall))
    candidate_count_overall, (log_norm, question_count_overall) = lax.scan(per_block, jnp.zeros((BATCH, D), jnp.float32), q_blocks)
    log_norm = log_norm.reshape(BATCH)
    question_count_overall = question_count_overall.reshape(BATCH, D)
    loss = jnp.mean(log_norm - matching_score)
    question_slope = direction_slope((question_count_overall - candidate_gathered_all) / softmax_sharpness, question_direction, question_magnitude)
    candidate_slope = direction_slope((candidate_count_overall - question_gathered_all) / softmax_sharpness, candidate_direction, candidate_magnitude)
    return (loss, question_slope, candidate_slope)
```

```python
import functools

import jax
import jax.numpy as jnp
from jax import lax
from jax.experimental import pallas as pl
from jax.experimental.pallas import tpu as pltpu
from jax.sharding import PartitionSpec as P

MESH = pl.DeviceIdType.MESH
ROWS = 128
D = 256
BATCH = 16384
INV_TEMP = 20.0
TINY = 1e-12
F32 = jnp.float32
BF16 = jnp.bfloat16
ORDER = (7, 3, 5, 6, 1, 2, 4)


def flip_low(p, d):
    return p + 1 - 2 * (p % 2) if d else p


def flip_high(p, d):
    return 3 - p if d else p


def low_bit(p):
    return ((p + 1) // 2) % 2


def high_bit(p):
    return p // 2


def kernel(
    q_hbm,
    v_hbm,
    loss_ref,
    qs_ref,
    cs_ref,
    q_in,
    v_in,
    q_unit,
    v_unit,
    lens,
    qbuf,
    vbuf,
    t_ref,
    sbuf,
    ub,
    ud,
    us,
    ur,
    qsc,
    wb,
    w_own,
    wr,
    xbuf,
    ybuf,
    in_sem,
    q_send,
    q_recv,
    f_send,
    f_recv,
    v_send,
    v_recv,
    s_send,
    s_recv,
    d_sem,
    u_send,
    u_recv,
    w_send,
    w_recv,
    x_send,
    x_recv,
    y_send,
    y_recv,
):
    core = lax.axis_index("blk")
    other = 1 - core
    dp = lax.axis_index("dp")
    z, y, x = dp // 16, (dp // 4) % 4, dp % 4

    def chip_a(k):
        zz = flip_low(z, (k >> 2) & 1)
        yy = flip_low(y, (k >> 1) & 1)
        xx = flip_low(x, k & 1)
        return zz * 16 + yy * 4 + xx, low_bit(zz) * 4 + low_bit(yy) * 2 + low_bit(xx)

    def chip_b(k):
        zz = flip_high(z, (k >> 2) & 1)
        yy = flip_high(y, (k >> 1) & 1)
        xx = flip_high(x, k & 1)
        return zz * 16 + yy * 4 + xx

    a_chip = [chip_a(k) for k in range(8)]
    b_chip = [chip_b(k) for k in range(8)]
    c_me = a_chip[0][1]
    b_me = high_bit(z) * 4 + high_bit(y) * 2 + high_bit(x)
    lo = pl.multiple_of(core * ROWS, ROWS)

    copies = []

    def send(src, dst, ssem, rsem, blk, chip):
        copy = pltpu.make_async_remote_copy(
            src_ref=src, dst_ref=dst, send_sem=ssem, recv_sem=rsem, device_id=(blk, chip), device_id_type=MESH
        )
        copy.start()
        copies.append(copy)
        return copy

    barrier = pltpu.get_barrier_semaphore()
    for k in ORDER:
        for blk in (core, other):
            pl.semaphore_signal(barrier, inc=1, device_id=(blk, a_chip[k][0]), device_id_type=MESH)
        pl.semaphore_signal(barrier, inc=1, device_id=(core, b_chip[k]), device_id_type=MESH)
    pl.semaphore_signal(barrier, inc=1, device_id=(other, dp), device_id_type=MESH)

    load_q = pltpu.make_async_copy(q_hbm, q_in, in_sem.at[0])
    load_v = pltpu.make_async_copy(v_hbm, v_in, in_sem.at[1])
    load_q.start()
    load_v.start()
    load_q.wait()
    load_v.wait()

    def unit_rows(value):
        wide = value.astype(F32)
        length = jnp.sqrt(jnp.sum(wide * wide, axis=1, keepdims=True) + TINY)
        return wide / length, length

    qu, ql = unit_rows(q_in[...])
    vu, vl = unit_rows(v_in[...])
    q_hat, v_hat = qu.astype(BF16), vu.astype(BF16)
    q_unit[...] = qu
    v_unit[...] = vu
    lens[0] = ql
    lens[1] = vl
    q_own = qbuf.at[c_me, pl.ds(lo, ROWS)]
    qbuf[c_me, pl.ds(lo, ROWS), :] = q_hat
    vbuf[0] = v_hat
    hits = jnp.sum(q_hat.astype(F32) * v_hat.astype(F32), axis=0, keepdims=True)
    positive = (hits[:, :ROWS] + hits[:, ROWS:]) * INV_TEMP

    pl.semaphore_wait(barrier, 22)

    send(q_own, q_own, f_send.at[0], f_recv.at[0], other, dp)
    q_in_flight, v_in_flight = {}, {}
    for k in ORDER:
        q_in_flight[k] = send(q_own, q_own, q_send.at[k], q_recv.at[k], core, a_chip[k][0])
        v_in_flight[k] = send(vbuf.at[0], vbuf.at[k], v_send.at[k], v_recv.at[k], core, b_chip[k])

    for k in (1, 2, 4, 3, 5, 6, 7):
        theirs = qbuf.at[a_chip[k][1], pl.ds(lo, ROWS)]
        q_in_flight[k].wait_recv()
        send(theirs, theirs, f_send.at[k], f_recv.at[k], other, dp)
    for k in ORDER:
        v_in_flight[k].wait_recv()

    def wait_forward(k):
        theirs = qbuf.at[a_chip[k][1], pl.ds(lo, ROWS)]
        pltpu.make_async_remote_copy(
            src_ref=theirs,
            dst_ref=theirs,
            send_sem=f_send.at[k],
            recv_sem=f_recv.at[k],
            device_id=(other, dp),
            device_id_type=MESH,
        ).wait_recv()

    for k in range(8):
        wait_forward(k)

    v_all = vbuf[...].reshape(8 * ROWS, D)
    a_me = core * 8 + c_me
    for c in range(8):
        logits = lax.dot_general(v_all, qbuf[c], (((1,), (1,)), ((), ())), preferred_element_type=F32)
        e = jnp.exp(logits * INV_TEMP)
        sbuf[a_me, pl.ds(c, 1), :] = jnp.sum(e, axis=0, keepdims=True)
        t_ref[c] = e.astype(BF16)

    s_own = sbuf.at[a_me]
    s_copies = [send(s_own, s_own, s_send.at[0], s_recv.at[0], other, dp)]
    for k in ORDER:
        for i, blk in enumerate((core, other)):
            s_copies.append(send(s_own, s_own, s_send.at[2 * k + i], s_recv.at[2 * k + i], blk, a_chip[k][0]))

    for c in range(8):
        ut = lax.dot_general(v_all, t_ref[c], (((0,), (0,)), ((), ())), preferred_element_type=F32)
        ub[0, c] = ut[:, :ROWS].astype(BF16)
        ub[1, c] = ut[:, ROWS:].astype(BF16)
    across = send(ub.at[other], ud, d_sem.at[0], d_sem.at[1], other, dp)

    for copy in s_copies:
        copy.wait_recv()
    total = sbuf[0]
    for a in range(1, 16):
        total = total + sbuf[a]
    inverse = jnp.transpose(1.0 / total)
    for c in range(8):
        qsc[c] = (qbuf[c].astype(F32) * inverse[:, c : c + 1]).astype(BF16)

    w_copies = []
    for half in (1, 0):
        acc = jnp.zeros((4 * ROWS, D), F32)
        for c in range(8):
            acc = acc + jnp.dot(t_ref[c, half * 512 : half * 512 + 512, :], qsc[c], preferred_element_type=F32)
        for j in (3, 2, 1, 0):
            k = half * 4 + j
            part = acc[j * ROWS : (j + 1) * ROWS]
            if k == 0:
                w_own[...] = part
            else:
                wb[k] = part.astype(BF16)
                w_copies.append(send(wb.at[k], wr.at[k], w_send.at[k], w_recv.at[k], core, b_chip[k]))

    mine = lax.broadcasted_iota(jnp.int32, total.shape, 0) == c_me
    s_row = jnp.sum(jnp.where(mine, total, 0.0), axis=0, keepdims=True)
    s_row = jnp.where(core == 0, s_row[:, :ROWS], s_row[:, ROWS:])
    xbuf[b_me] = jnp.zeros((8, ROWS), F32)
    xbuf[b_me, 0:1, :] = jnp.log(s_row) - positive
    x_copies = [
        send(xbuf.at[b_me], xbuf.at[b_me], x_send.at[k], x_recv.at[k], core, b_chip[k]) for k in ORDER
    ]

    across.wait_recv()
    for c in range(8):
        us[c] = (ub[core, c].astype(F32) + ud[c].astype(F32)).astype(BF16)
    u_copies = [
        send(us.at[a_chip[k][1]], ur.at[k], u_send.at[k], u_recv.at[k], core, a_chip[k][0]) for k in ORDER
    ]

    for copy in x_copies:
        copy.wait_recv()
    x_sum = xbuf[0]
    for b in range(1, 8):
        x_sum = x_sum + xbuf[b]
    ybuf[a_me] = x_sum
    y_copies = [send(ybuf.at[a_me], ybuf.at[a_me], y_send.at[0], y_recv.at[0], other, dp)]
    for k in ORDER:
        for i, blk in enumerate((core, other)):
            y_copies.append(
                send(ybuf.at[a_me], ybuf.at[a_me], y_send.at[2 * k + i], y_recv.at[2 * k + i], blk, a_chip[k][0])
            )

    def slope(pull, unit, length):
        along = jnp.sum(unit * pull, axis=1, keepdims=True)
        return (pull - unit * along) / length

    for copy in u_copies:
        copy.wait_recv()
    u_sum = ub[core, c_me].astype(F32) + ud[c_me].astype(F32)
    for k in range(1, 8):
        u_sum = u_sum + ur[k].astype(F32)
    q_pull = (jnp.transpose(u_sum / s_row) - vbuf[0].astype(F32)) * INV_TEMP
    qs_ref[...] = slope(q_pull, q_unit[...], lens[0])

    for copy in w_copies:
        copy.wait_recv()
    w_sum = w_own[...]
    for k in range(1, 8):
        w_sum = w_sum + wr[k].astype(F32)
    v_pull = (w_sum - qbuf[c_me, pl.ds(lo, ROWS), :].astype(F32)) * INV_TEMP
    cs_ref[...] = slope(v_pull, v_unit[...], lens[1])

    for copy in y_copies:
        copy.wait_recv()
    y_sum = ybuf[0]
    for a in range(1, 16):
        y_sum = y_sum + ybuf[a]
    loss_ref[0, 0] = jnp.sum(y_sum) / BATCH

    for copy in copies:
        copy.wait_send()


def per_device(queries, items):
    dma = pltpu.SemaphoreType.DMA
    vmem = pltpu.VMEM
    loss, q_slope, v_slope = pl.pallas_call(
        kernel,
        out_shape=(
            jax.ShapeDtypeStruct((1, 1), F32),
            jax.ShapeDtypeStruct((ROWS, D), F32),
            jax.ShapeDtypeStruct((ROWS, D), F32),
        ),
        in_specs=[pl.BlockSpec(memory_space=pl.ANY)] * 2,
        out_specs=(
            pl.BlockSpec(memory_space=pltpu.SMEM),
            pl.BlockSpec(memory_space=pltpu.VMEM),
            pl.BlockSpec(memory_space=pltpu.VMEM),
        ),
        scratch_shapes=[
            vmem((ROWS, D), BF16),
            vmem((ROWS, D), BF16),
            vmem((ROWS, D), F32),
            vmem((ROWS, D), F32),
            vmem((2, ROWS, 1), F32),
            vmem((8, 2 * ROWS, D), BF16),
            vmem((8, ROWS, D), BF16),
            vmem((8, 8 * ROWS, 2 * ROWS), BF16),
            vmem((16, 8, 2 * ROWS), F32),
            vmem((2, 8, D, ROWS), BF16),
            vmem((8, D, ROWS), BF16),
            vmem((8, D, ROWS), BF16),
            vmem((8, D, ROWS), BF16),
            vmem((8, 2 * ROWS, D), BF16),
            vmem((8, ROWS, D), BF16),
            vmem((ROWS, D), F32),
            vmem((8, ROWS, D), BF16),
            vmem((8, 8, ROWS), F32),
            vmem((16, 8, ROWS), F32),
            dma((2,)),
            dma((8,)),
            dma((8,)),
            dma((8,)),
            dma((8,)),
            dma((8,)),
            dma((8,)),
            dma((16,)),
            dma((16,)),
            dma((2,)),
            dma((8,)),
            dma((8,)),
            dma((8,)),
            dma((8,)),
            dma((8,)),
            dma((8,)),
            dma((16,)),
            dma((16,)),
        ],
        compiler_params=pltpu.CompilerParams(collective_id=0, has_side_effects=True),
    )(queries, items)
    return loss.reshape(()), q_slope, v_slope


def solution(mesh):
    spec = P(("blk", "dp"), None)
    return jax.shard_map(
        per_device, mesh=mesh, in_specs=(spec, spec), out_specs=(P(), spec, spec), check_vma=False
    )
```

```python
import functools

import jax
import jax.numpy as jnp
from jax import lax
from jax.experimental import pallas as pl
from jax.experimental.pallas import tpu as pltpu
from jax.sharding import PartitionSpec as P

MESH = pl.DeviceIdType.MESH
ROWS = 128
D = 256
BATCH = 16384
INV_TEMP = 20.0
TINY = 1e-12
F32 = jnp.float32
BF16 = jnp.bfloat16
ORDER = (7, 3, 5, 6, 1, 2, 4)


def flip_low(p, d):
    return p + 1 - 2 * lax.rem(p, 2) if d else p


def flip_high(p, d):
    return 3 - p if d else p


def low_bit(p):
    return lax.rem(lax.div(p + 1, 2), 2)


def high_bit(p):
    return lax.div(p, 2)


def kernel(
    q_hbm,
    v_hbm,
    hits_ref,
    qs_ref,
    cs_ref,
    q_in,
    v_in,
    q_unit,
    v_unit,
    lens,
    qbuf,
    vbuf,
    t_ref,
    sbuf,
    ub,
    ud,
    us,
    ur,
    qsc,
    wb,
    w_own,
    wr,
    xbuf,
    ybuf,
    in_sem,
    q_send,
    q_recv,
    f_send,
    f_recv,
    v_send,
    v_recv,
    s_send,
    s_recv,
    d_sem,
    u_send,
    u_recv,
    w_send,
    w_recv,
    x_send,
    x_recv,
    y_send,
    y_recv,
    near_sem,
    far_sem,
):
    core = lax.axis_index("blk")
    other = 1 - core
    dp = lax.axis_index("dp")
    z, y, x = lax.div(dp, 16), lax.rem(lax.div(dp, 4), 4), lax.rem(dp, 4)

    def chip_a(k):
        zz = flip_low(z, (k >> 2) & 1)
        yy = flip_low(y, (k >> 1) & 1)
        xx = flip_low(x, k & 1)
        return zz * 16 + yy * 4 + xx, low_bit(zz) * 4 + low_bit(yy) * 2 + low_bit(xx)

    def chip_b(k):
        zz = flip_high(z, (k >> 2) & 1)
        yy = flip_high(y, (k >> 1) & 1)
        xx = flip_high(x, k & 1)
        return zz * 16 + yy * 4 + xx

    a_chip = [chip_a(k) for k in range(8)]
    b_chip = [chip_b(k) for k in range(8)]
    c_me = a_chip[0][1]
    b_me = high_bit(z) * 4 + high_bit(y) * 2 + high_bit(x)
    lo = pl.multiple_of(core * ROWS, ROWS)

    copies = []

    def send(src, dst, ssem, rsem, blk, chip):
        copy = pltpu.make_async_remote_copy(
            src_ref=src, dst_ref=dst, send_sem=ssem, recv_sem=rsem, device_id=(blk, chip), device_id_type=MESH
        )
        copy.start()
        copies.append(copy)
        return copy

    barrier = pltpu.get_barrier_semaphore()

    def tell(sem, blk, chip):
        pl.semaphore_signal(sem, inc=1, device_id=(blk, chip), device_id_type=MESH)

    for d in range(3):
        tell(barrier, core, a_chip[1 << d][0])
        tell(barrier, core, b_chip[1 << d])
    tell(barrier, other, dp)

    load_q = pltpu.make_async_copy(q_hbm, q_in, in_sem.at[0])
    load_v = pltpu.make_async_copy(v_hbm, v_in, in_sem.at[1])
    load_q.start()
    load_v.start()
    load_q.wait()
    load_v.wait()

    def unit_rows(value):
        wide = value.astype(F32)
        length = jnp.sqrt(jnp.sum(wide * wide, axis=1, keepdims=True) + TINY)
        return wide / length, length

    qu, ql = unit_rows(q_in[...])
    vu, vl = unit_rows(v_in[...])
    q_hat, v_hat = qu.astype(BF16), vu.astype(BF16)
    q_unit[...] = qu
    v_unit[...] = vu
    lens[0] = ql
    lens[1] = vl
    q_own = qbuf.at[c_me, pl.ds(lo, ROWS)]
    qbuf[c_me, pl.ds(lo, ROWS), :] = q_hat
    vbuf[0] = v_hat
    hits = jnp.sum(q_hat.astype(F32) * v_hat.astype(F32), axis=0, keepdims=True)
    ybuf[core * 8 + c_me] = jnp.broadcast_to(hits[:, :ROWS] + hits[:, ROWS:], (8, ROWS))

    pl.semaphore_wait(barrier, 7)
    for d in range(3):
        tell(near_sem.at[d], core, a_chip[1 << d][0])
        tell(near_sem.at[3 + d], core, b_chip[1 << d])

    q_flight, v_flight, f_flight = {}, {}, {}

    def gather(k):
        q_flight[k] = send(q_own, q_own, q_send.at[k], q_recv.at[k], core, a_chip[k][0])
        v_flight[k] = send(vbuf.at[0], vbuf.at[k], v_send.at[k], v_recv.at[k], core, b_chip[k])

    f_flight[0] = send(q_own, q_own, f_send.at[0], f_recv.at[0], other, dp)
    for k in (1, 2, 4):
        gather(k)
    for d in range(6):
        pl.semaphore_wait(near_sem.at[d], 1)
    tell(far_sem.at[0], core, a_chip[1][0])
    tell(far_sem.at[1], core, b_chip[1])
    for k in (3, 5, 6):
        gather(k)
    for d in range(2):
        pl.semaphore_wait(far_sem.at[d], 1)
    gather(7)

    for k in (1, 2, 4, 3, 5, 6, 7):
        theirs = qbuf.at[a_chip[k][1], pl.ds(lo, ROWS)]
        q_flight[k].wait_recv()
        f_flight[k] = send(theirs, theirs, f_send.at[k], f_recv.at[k], other, dp)
    for k in range(1, 8):
        v_flight[k].wait_recv()

    for k in range(8):
        f_flight[k].wait_recv()

    v_all = vbuf[...].reshape(8 * ROWS, D)
    a_me = core * 8 + c_me
    for c in range(8):
        logits = lax.dot_general(v_all, qbuf[c], (((1,), (1,)), ((), ())), preferred_element_type=F32)
        e = jnp.exp(logits * INV_TEMP)
        sbuf[a_me, pl.ds(c, 1), :] = jnp.sum(e, axis=0, keepdims=True)
        t_ref[c] = e.astype(BF16)

    def exchange(ref, ssem, rsem):
        flight = []
        for k in ORDER:
            for i, blk in enumerate((core, other)):
                n = 2 * k + i
                flight.append(send(ref, ref, ssem.at[n], rsem.at[n], blk, a_chip[k][0]))
        flight.append(send(ref, ref, ssem.at[0], rsem.at[0], other, dp))
        return flight

    s_flight = exchange(sbuf.at[a_me], s_send, s_recv)
    y_flight = exchange(ybuf.at[a_me], y_send, y_recv)

    for c in range(8):
        ut = lax.dot_general(v_all, t_ref[c], (((0,), (0,)), ((), ())), preferred_element_type=F32)
        ub[0, c] = ut[:, :ROWS].astype(BF16)
        ub[1, c] = ut[:, ROWS:].astype(BF16)
    across = send(ub.at[other], ud, d_sem.at[0], d_sem.at[1], other, dp)

    across.wait_recv()
    for c in range(8):
        us[c] = (ub[core, c].astype(F32) + ud[c].astype(F32)).astype(BF16)
    u_flight = [
        send(us.at[a_chip[k][1]], ur.at[k], u_send.at[k], u_recv.at[k], core, a_chip[k][0]) for k in ORDER
    ]

    for copy in s_flight:
        copy.wait_recv()
    total = sbuf[0]
    for a in range(1, 16):
        total = total + sbuf[a]
    inverse = jnp.transpose(1.0 / total)
    for c in range(8):
        qsc[c] = (qbuf[c].astype(F32) * inverse[:, c : c + 1]).astype(BF16)

    for copy in y_flight:
        copy.wait_recv()
    hits = ybuf[0]
    for a in range(1, 16):
        hits = hits + ybuf[a]
    logs = jnp.log(total)
    xbuf[b_me] = (logs[:, :ROWS] + logs[:, ROWS:]) - hits * (INV_TEMP / 8.0)
    x_flight = [
        send(xbuf.at[b_me], xbuf.at[b_me], x_send.at[k], x_recv.at[k], core, b_chip[k]) for k in ORDER
    ]

    w_flight = []
    for half in (1, 0):
        acc = jnp.zeros((4 * ROWS, D), F32)
        for c in range(8):
            acc = acc + jnp.dot(t_ref[c, half * 512 : half * 512 + 512, :], qsc[c], preferred_element_type=F32)
        for j in (3, 2, 1, 0):
            k = half * 4 + j
            part = acc[j * ROWS : (j + 1) * ROWS]
            if k == 0:
                w_own[...] = part
            else:
                wb[k] = part.astype(BF16)
                w_flight.append(send(wb.at[k], wr.at[k], w_send.at[k], w_recv.at[k], core, b_chip[k]))

    mine = lax.broadcasted_iota(jnp.int32, total.shape, 0) == c_me
    s_row = jnp.sum(jnp.where(mine, total, 0.0), axis=0, keepdims=True)
    s_row = jnp.where(core == 0, s_row[:, :ROWS], s_row[:, ROWS:])

    def slope(pull, unit, length):
        along = jnp.sum(unit * pull, axis=1, keepdims=True)
        return (pull - unit * along) / length

    for copy in u_flight:
        copy.wait_recv()
    u_sum = ub[core, c_me].astype(F32) + ud[c_me].astype(F32)
    for k in range(1, 8):
        u_sum = u_sum + ur[k].astype(F32)
    q_pull = (jnp.transpose(u_sum / s_row) - vbuf[0].astype(F32)) * INV_TEMP
    qs_ref[...] = slope(q_pull, q_unit[...], lens[0])

    for copy in w_flight:
        copy.wait_recv()
    w_sum = w_own[...]
    for k in range(1, 8):
        w_sum = w_sum + wr[k].astype(F32)
    v_pull = (w_sum - qbuf[c_me, pl.ds(lo, ROWS), :].astype(F32)) * INV_TEMP
    cs_ref[...] = slope(v_pull, v_unit[...], lens[1])

    for copy in x_flight:
        copy.wait_recv()
    x_sum = xbuf[0]
    for b in range(1, 8):
        x_sum = x_sum + xbuf[b]
    hits_ref[...] = x_sum

    for copy in copies:
        copy.wait_send()


def write_out(l_ref, q_ref, v_ref, l_out, q_out, v_out, l_own, sem):
    q_copy = pltpu.make_async_copy(q_ref, q_out, sem.at[0])
    v_copy = pltpu.make_async_copy(v_ref, v_out, sem.at[1])
    q_copy.start()
    v_copy.start()
    l_own[0, 0] = jnp.sum(l_ref[...]) / BATCH
    l_copy = pltpu.make_async_copy(l_own, l_out, sem.at[2])
    l_copy.start()
    l_copy.wait()
    q_copy.wait()
    v_copy.wait()


def per_device(queries, items):
    dma = pltpu.SemaphoreType.DMA
    vmem = pltpu.VMEM
    parts = pl.pallas_call(
        kernel,
        out_shape=(vmem((8, ROWS), F32), vmem((ROWS, D), F32), vmem((ROWS, D), F32)),
        in_specs=[pl.BlockSpec(memory_space=pltpu.HBM)] * 2,
        out_specs=(pl.BlockSpec(memory_space=vmem),) * 3,
        scratch_shapes=[
            vmem((ROWS, D), BF16),
            vmem((ROWS, D), BF16),
            vmem((ROWS, D), F32),
            vmem((ROWS, D), F32),
            vmem((2, ROWS, 1), F32),
            vmem((8, 2 * ROWS, D), BF16),
            vmem((8, ROWS, D), BF16),
            vmem((8, 8 * ROWS, 2 * ROWS), BF16),
            vmem((16, 8, 2 * ROWS), F32),
            vmem((2, 8, D, ROWS), BF16),
            vmem((8, D, ROWS), BF16),
            vmem((8, D, ROWS), BF16),
            vmem((8, D, ROWS), BF16),
            vmem((8, 2 * ROWS, D), BF16),
            vmem((8, ROWS, D), BF16),
            vmem((ROWS, D), F32),
            vmem((8, ROWS, D), BF16),
            vmem((8, 8, ROWS), F32),
            vmem((16, 8, ROWS), F32),
            dma((2,)),
            dma((8,)),
            dma((8,)),
            dma((8,)),
            dma((8,)),
            dma((8,)),
            dma((8,)),
            dma((16,)),
            dma((16,)),
            dma((2,)),
            dma((8,)),
            dma((8,)),
            dma((8,)),
            dma((8,)),
            dma((8,)),
            dma((8,)),
            dma((16,)),
            dma((16,)),
            pltpu.SemaphoreType.REGULAR((6,)),
            pltpu.SemaphoreType.REGULAR((2,)),
        ],
        compiler_params=pltpu.CompilerParams(collective_id=0, has_side_effects=True),
    )(queries, items)
    loss, q_slope, v_slope = pl.pallas_call(
        write_out,
        out_shape=(
            jax.ShapeDtypeStruct((1, 1), F32),
            jax.ShapeDtypeStruct((ROWS, D), F32),
            jax.ShapeDtypeStruct((ROWS, D), F32),
        ),
        in_specs=[pl.BlockSpec(memory_space=vmem)] * 3,
        out_specs=(
            pl.BlockSpec(memory_space=pltpu.HBM),
            pl.BlockSpec(memory_space=pltpu.HBM),
            pl.BlockSpec(memory_space=pltpu.HBM),
        ),
        scratch_shapes=[pltpu.SMEM((1, 1), F32), dma((3,))],
        compiler_params=pltpu.CompilerParams(vmem_limit_bytes=1024 * 1024),
    )(*(pltpu.with_memory_space_constraint(part, vmem) for part in parts))
    return loss.reshape(()), q_slope, v_slope


def solution(mesh):
    spec = P(("blk", "dp"), None)
    return jax.shard_map(
        per_device, mesh=mesh, in_specs=(spec, spec), out_specs=(P(), spec, spec), check_vma=False
    )
```

```python
import jax
import jax.numpy as jnp
from jax import lax
from jax.experimental import pallas as pl
from jax.experimental.pallas import tpu as pltpu
from jax.sharding import PartitionSpec as P

MESH = pl.DeviceIdType.MESH
ROWS = 128
D = 256
BATCH = 16384
INV_TEMP = 20.0
TINY = 1e-12
F32 = jnp.float32
BF16 = jnp.bfloat16
A_LOW = (True, True, True)
SLOT = (0, 1, 2, 4, 3, 5, 6, 7)
NEAR, FAR = (0, 1, 2, 4), (3, 5, 6, 7)
ORDER = (7, 3, 5, 6, 1, 2, 4)


def flip_low(p, d):
    return p + 1 - 2 * lax.rem(p, 2) if d else p


def flip_high(p, d):
    return 3 - p if d else p


def low_bit(p):
    return lax.rem(lax.div(p + 1, 2), 2)


def high_bit(p):
    return lax.div(p, 2)


def kernel(
    q_hbm,
    v_hbm,
    hits_ref,
    qs_ref,
    cs_ref,
    q_in,
    v_in,
    q_unit,
    v_unit,
    lens,
    qbuf,
    vbuf,
    t_ref,
    sbuf,
    spart,
    ub,
    ud,
    us,
    ur,
    qsc,
    wb,
    w_own,
    wr,
    xbuf,
    ybuf,
    in_sem,
    q_send,
    q_recv,
    f_send,
    f_recv,
    v_send,
    v_recv,
    s_send,
    s_recv,
    d_sem,
    u_send,
    u_recv,
    w_send,
    w_recv,
    x_send,
    x_recv,
    y_send,
    y_recv,
    near_sem,
    far_sem,
    side_sem,
):
    core = lax.axis_index("blk")
    other = 1 - core
    dp = lax.axis_index("dp")
    z, y, x = lax.div(dp, 16), lax.rem(lax.div(dp, 4), 4), lax.rem(dp, 4)

    place = (z, y, x)

    def partner(k, low):
        steps = ((k >> 2) & 1, (k >> 1) & 1, k & 1)
        zz, yy, xx = (
            (flip_low if is_low == low else flip_high)(p, d) for p, d, is_low in zip(place, steps, A_LOW)
        )
        return zz, yy, xx

    def rank(place, low):
        bits = [(low_bit if is_low == low else high_bit)(p) for p, is_low in zip(place, A_LOW)]
        return bits[0] * 4 + bits[1] * 2 + bits[2]

    def number(place):
        return place[0] * 16 + place[1] * 4 + place[2]

    a_chip = [(number(partner(k, True)), rank(partner(k, True), True)) for k in range(8)]
    b_chip = [number(partner(k, False)) for k in range(8)]
    c_me = a_chip[0][1]
    b_me = rank(place, False)
    lo = pl.multiple_of(core * ROWS, ROWS)

    copies = []

    def plan(src, dst, ssem, rsem, blk, chip):
        return pltpu.make_async_remote_copy(
            src_ref=src, dst_ref=dst, send_sem=ssem, recv_sem=rsem, device_id=(blk, chip), device_id_type=MESH
        )

    def send(*where):
        copy = plan(*where)
        copy.start()
        copies.append(copy)
        return copy

    barrier = pltpu.get_barrier_semaphore()

    def tell(sem, blk, chip):
        pl.semaphore_signal(sem, inc=1, device_id=(blk, chip), device_id_type=MESH)

    for d in range(3):
        tell(barrier, core, a_chip[1 << d][0])
        tell(barrier, core, b_chip[1 << d])
    tell(barrier, other, dp)

    load_q = pltpu.make_async_copy(q_hbm, q_in, in_sem.at[0])
    load_v = pltpu.make_async_copy(v_hbm, v_in, in_sem.at[1])
    load_q.start()
    load_v.start()
    load_q.wait()
    load_v.wait()

    def unit_rows(value):
        wide = value.astype(F32)
        length = jnp.sqrt(jnp.sum(wide * wide, axis=1, keepdims=True) + TINY)
        return wide / length, length

    qu, ql = unit_rows(q_in[...])
    vu, vl = unit_rows(v_in[...])
    q_hat, v_hat = qu.astype(BF16), vu.astype(BF16)
    q_unit[...] = qu
    v_unit[...] = vu
    lens[0] = ql
    lens[1] = vl
    q_own = qbuf.at[c_me, pl.ds(lo, ROWS)]
    qbuf[c_me, pl.ds(lo, ROWS), :] = q_hat
    vbuf[0] = v_hat
    hits = jnp.sum(q_hat.astype(F32) * v_hat.astype(F32), axis=0, keepdims=True)
    ybuf[core * 8 + c_me] = hits[:, :ROWS] + hits[:, ROWS:]

    pl.semaphore_wait(barrier, 7)
    for d in range(3):
        tell(near_sem.at[d], core, a_chip[1 << d][0])
        tell(near_sem.at[3 + d], core, b_chip[1 << d])

    q_flight, v_flight, f_flight = {}, {}, {}

    def gather_q(k):
        q_flight[k] = send(q_own, q_own, q_send.at[k], q_recv.at[k], core, a_chip[k][0])

    def gather_v(k):
        v_flight[k] = send(vbuf.at[0], vbuf.at[SLOT[k]], v_send.at[k], v_recv.at[k], core, b_chip[k])

    f_flight[0] = send(q_own, q_own, f_send.at[0], f_recv.at[0], other, dp)
    for k in (1, 2, 4):
        gather_v(k)
        gather_q(k)
    for d in range(3):
        pl.semaphore_wait(near_sem.at[d], 1)
    tell(far_sem.at[0], core, a_chip[1][0])
    for k in (3, 5, 6):
        gather_q(k)
    for d in range(3, 6):
        pl.semaphore_wait(near_sem.at[d], 1)
    tell(far_sem.at[1], core, b_chip[1])
    for k in (3, 5, 6):
        gather_v(k)
    pl.semaphore_wait(far_sem.at[0], 1)
    gather_q(7)
    pl.semaphore_wait(far_sem.at[1], 1)
    gather_v(7)
    tell(side_sem, other, dp)
    pl.semaphore_wait(side_sem, 1)
    f_flight[7] = send(q_own, q_own, f_send.at[7], f_recv.at[7], other, a_chip[7][0])

    def pass_on(ks):
        for k in ks:
            theirs = qbuf.at[a_chip[k][1], pl.ds(lo, ROWS)]
            q_flight[k].wait_recv()
            f_flight[k] = send(theirs, theirs, f_send.at[k], f_recv.at[k], other, dp)

    def weigh(half, ks):
        rows = slice(half * 512, half * 512 + 512)
        v_half = vbuf[half * 4 : half * 4 + 4].reshape(512, D)
        for k in ks:
            c = a_chip[k][1]
            logits = lax.dot_general(v_half, qbuf[c], (((1,), (1,)), ((), ())), preferred_element_type=F32)
            e = jnp.exp(logits * INV_TEMP)
            spart[half, c, 0:1, :] = jnp.sum(e, axis=0, keepdims=True)
            t_ref[c, rows, :] = e.astype(BF16)

    pass_on(NEAR[1:])
    for k in NEAR[1:]:
        v_flight[k].wait_recv()
    for k in NEAR:
        f_flight[k].wait_recv()
    weigh(0, NEAR)
    pass_on(FAR[:3])
    q_flight[7].wait_recv()
    for k in FAR:
        f_flight[k].wait_recv()
    weigh(0, FAR)
    for k in FAR:
        v_flight[k].wait_recv()
    weigh(1, range(8))
    a_me = core * 8 + c_me
    for c in range(8):
        sbuf[a_me, c : c + 1, :] = spart[0, c, 0:1, :] + spart[1, c, 0:1, :]
    v_all = vbuf[...].reshape(8 * ROWS, D)

    def exchange(ref, ssem, rsem):
        flight = []
        for k in ORDER:
            for i, blk in enumerate((core, other)):
                n = 2 * k + i
                flight.append(send(ref, ref, ssem.at[n], rsem.at[n], blk, a_chip[k][0]))
        flight.append(send(ref, ref, ssem.at[0], rsem.at[0], other, dp))
        return flight

    s_flight = exchange(sbuf.at[a_me], s_send, s_recv)
    y_flight = exchange(ybuf.at[a_me], y_send, y_recv)

    for c in range(8):
        ut = lax.dot_general(v_all, t_ref[c], (((0,), (0,)), ((), ())), preferred_element_type=F32)
        ub[0, c] = ut[:, :ROWS].astype(BF16)
        ub[1, c] = ut[:, ROWS:].astype(BF16)
    across = send(ub.at[other], ud, d_sem.at[0], d_sem.at[1], other, dp)

    across.wait_recv()
    for c in range(8):
        us[c] = (ub[core, c].astype(F32) + ud[c].astype(F32)).astype(BF16)
    u_flight = [
        send(us.at[a_chip[k][1]], ur.at[k], u_send.at[k], u_recv.at[k], core, a_chip[k][0]) for k in ORDER
    ]

    for copy in s_flight:
        copy.wait_recv()
    total = sbuf[0]
    for a in range(1, 16):
        total = total + sbuf[a]
    inverse = jnp.transpose(1.0 / total)
    for c in range(8):
        qsc[c] = (qbuf[c].astype(F32) * inverse[:, c : c + 1]).astype(BF16)

    x_flight = []

    def loss_rows():
        for copy in y_flight:
            copy.wait_recv()
        hits = ybuf[0]
        for a in range(1, 16):
            hits = hits + ybuf[a]
        logs = jnp.sum(jnp.log(total), axis=0, keepdims=True)
        xbuf[b_me] = (logs[:, :ROWS] + logs[:, ROWS:]) - hits * INV_TEMP
        for k in ORDER:
            x_flight.append(send(xbuf.at[b_me], xbuf.at[b_me], x_send.at[k], x_recv.at[k], core, b_chip[k]))

    w_flight = {
        k: plan(wb.at[k], wr.at[k], w_send.at[k], w_recv.at[k], core, b_chip[k]) for k in range(1, 8)
    }

    def w_chunk(quarter):
        rows = slice(quarter * 256, quarter * 256 + 256)
        acc = jnp.dot(t_ref[0, rows, :], qsc[0], preferred_element_type=F32)
        for c in range(1, 8):
            acc = acc + jnp.dot(t_ref[c, rows, :], qsc[c], preferred_element_type=F32)
        for j in (1, 0):
            k = SLOT[quarter * 2 + j]
            part = acc[j * ROWS : (j + 1) * ROWS]
            if k == 0:
                w_own[...] = part
            else:
                wb[k] = part.astype(BF16)
                w_flight[k].start()

    for quarter in (3, 2, 1, 0):
        w_chunk(quarter)
        if quarter == 3:
            loss_rows()

    mine = lax.broadcasted_iota(jnp.int32, total.shape, 0) == c_me
    s_row = jnp.sum(jnp.where(mine, total, 0.0), axis=0, keepdims=True)
    s_row = jnp.where(core == 0, s_row[:, :ROWS], s_row[:, ROWS:])

    def slope(pull, unit, length):
        along = jnp.sum(unit * pull, axis=1, keepdims=True)
        return (pull - unit * along) / length

    for copy in u_flight:
        copy.wait_recv()
    u_sum = ub[core, c_me].astype(F32) + ud[c_me].astype(F32)
    for k in range(1, 8):
        u_sum = u_sum + ur[k].astype(F32)
    q_pull = (jnp.transpose(u_sum / s_row) - vbuf[0].astype(F32)) * INV_TEMP
    qs_ref[...] = slope(q_pull, q_unit[...], lens[0])

    for copy in x_flight:
        copy.wait_recv()
    x_sum = xbuf[0]
    for b in range(1, 8):
        x_sum = x_sum + xbuf[b]
    hits_ref[...] = x_sum

    for copy in copies + list(w_flight.values()):
        copy.wait_send()

    for k in range(1, 8):
        w_flight[k].wait_recv()
    w_sum = w_own[...]
    for k in range(1, 8):
        w_sum = w_sum + wr[k].astype(F32)
    v_pull = (w_sum - qbuf[c_me, pl.ds(lo, ROWS), :].astype(F32)) * INV_TEMP
    cs_ref[...] = slope(v_pull, v_unit[...], lens[1])


def write_out(l_ref, q_ref, v_ref, l_out, q_out, v_out, l_own, sem):
    q_copy = pltpu.make_async_copy(q_ref, q_out, sem.at[0])
    v_copy = pltpu.make_async_copy(v_ref, v_out, sem.at[1])
    q_copy.start()
    v_copy.start()
    l_own[0, 0] = jnp.sum(l_ref[...]) / BATCH
    l_copy = pltpu.make_async_copy(l_own, l_out, sem.at[2])
    l_copy.start()
    l_copy.wait()
    q_copy.wait()
    v_copy.wait()


def per_device(queries, items):
    dma = pltpu.SemaphoreType.DMA
    vmem = pltpu.VMEM
    parts = pl.pallas_call(
        kernel,
        out_shape=(vmem((1, ROWS), F32), vmem((ROWS, D), F32), vmem((ROWS, D), F32)),
        in_specs=[pl.BlockSpec(memory_space=pltpu.HBM)] * 2,
        out_specs=(pl.BlockSpec(memory_space=vmem),) * 3,
        scratch_shapes=[
            vmem((ROWS, D), BF16),
            vmem((ROWS, D), BF16),
            vmem((ROWS, D), F32),
            vmem((ROWS, D), F32),
            vmem((2, ROWS, 1), F32),
            vmem((8, 2 * ROWS, D), BF16),
            vmem((8, ROWS, D), BF16),
            vmem((8, 8 * ROWS, 2 * ROWS), BF16),
            vmem((16, 8, 2 * ROWS), F32),
            vmem((2, 8, 8, 2 * ROWS), F32),
            vmem((2, 8, D, ROWS), BF16),
            vmem((8, D, ROWS), BF16),
            vmem((8, D, ROWS), BF16),
            vmem((8, D, ROWS), BF16),
            vmem((8, 2 * ROWS, D), BF16),
            vmem((8, ROWS, D), BF16),
            vmem((ROWS, D), F32),
            vmem((8, ROWS, D), BF16),
            vmem((8, 1, ROWS), F32),
            vmem((16, 1, ROWS), F32),
            dma((2,)),
            dma((8,)),
            dma((8,)),
            dma((8,)),
            dma((8,)),
            dma((8,)),
            dma((8,)),
            dma((16,)),
            dma((16,)),
            dma((2,)),
            dma((8,)),
            dma((8,)),
            dma((8,)),
            dma((8,)),
            dma((8,)),
            dma((8,)),
            dma((16,)),
            dma((16,)),
            pltpu.SemaphoreType.REGULAR((6,)),
            pltpu.SemaphoreType.REGULAR((2,)),
            pltpu.SemaphoreType.REGULAR,
        ],
        compiler_params=pltpu.CompilerParams(collective_id=0, has_side_effects=True),
    )(queries, items)
    loss, q_slope, v_slope = pl.pallas_call(
        write_out,
        out_shape=(
            jax.ShapeDtypeStruct((1, 1), F32),
            jax.ShapeDtypeStruct((ROWS, D), F32),
            jax.ShapeDtypeStruct((ROWS, D), F32),
        ),
        in_specs=[pl.BlockSpec(memory_space=vmem)] * 3,
        out_specs=(
            pl.BlockSpec(memory_space=pltpu.HBM),
            pl.BlockSpec(memory_space=pltpu.HBM),
            pl.BlockSpec(memory_space=pltpu.HBM),
        ),
        scratch_shapes=[pltpu.SMEM((1, 1), F32), dma((3,))],
        compiler_params=pltpu.CompilerParams(vmem_limit_bytes=1024 * 1024),
    )(*(pltpu.with_memory_space_constraint(part, vmem) for part in parts))
    return loss.reshape(()), q_slope, v_slope


def solution(mesh):
    spec = P(("blk", "dp"), None)
    return jax.shard_map(
        per_device, mesh=mesh, in_specs=(spec, spec), out_specs=(P(), spec, spec), check_vma=False
    )
```

```python
import jax
import jax.numpy as jnp
from jax import lax
from jax.experimental import pallas as pl
from jax.experimental.pallas import tpu as pltpu
from jax.sharding import PartitionSpec as P

MESH = pl.DeviceIdType.MESH
ROWS = 128
D = 256
BATCH = 16384
INV_TEMP = 20.0
TINY = 1e-12
F32 = jnp.float32
BF16 = jnp.bfloat16
A_LOW = (True, True, True)
SLOT = (0, 1, 2, 4, 3, 5, 6, 7)
NEAR, FAR = (0, 1, 2, 4), (3, 5, 6, 7)
V_WAVE = (None, 0, 0, 1, 0, 1, 1, 2)
ORDER = (7, 3, 5, 6, 1, 2, 4)


def flip_low(p, d):
    return p + 1 - 2 * lax.rem(p, 2) if d else p


def flip_high(p, d):
    return 3 - p if d else p


def low_bit(p):
    return lax.rem(lax.div(p + 1, 2), 2)


def high_bit(p):
    return lax.div(p, 2)


def kernel(
    q_hbm,
    v_hbm,
    hits_ref,
    qs_ref,
    cs_ref,
    q_in,
    v_in,
    q_unit,
    v_unit,
    lens,
    qbuf,
    vbuf,
    t_ref,
    sbuf,
    spart,
    ub,
    ud,
    us,
    ur,
    wb,
    w_own,
    wr,
    xbuf,
    ybuf,
    in_sem,
    q_send,
    q_recv,
    f_send,
    f_recv,
    v_send,
    v_recv,
    s_send,
    s_recv,
    d_send,
    d_recv,
    u_send,
    u_recv,
    w_send,
    w_recv,
    x_send,
    x_recv,
    y_send,
    y_recv,
    near_sem,
    far_sem,
    side_sem,
):
    core = lax.axis_index("blk")
    other = 1 - core
    dp = lax.axis_index("dp")
    z, y, x = lax.div(dp, 16), lax.rem(lax.div(dp, 4), 4), lax.rem(dp, 4)

    place = (z, y, x)

    def partner(k, low):
        steps = ((k >> 2) & 1, (k >> 1) & 1, k & 1)
        zz, yy, xx = (
            (flip_low if is_low == low else flip_high)(p, d) for p, d, is_low in zip(place, steps, A_LOW)
        )
        return zz, yy, xx

    def rank(place, low):
        bits = [(low_bit if is_low == low else high_bit)(p) for p, is_low in zip(place, A_LOW)]
        return bits[0] * 4 + bits[1] * 2 + bits[2]

    def number(place):
        return place[0] * 16 + place[1] * 4 + place[2]

    a_chip = [(number(partner(k, True)), rank(partner(k, True), True)) for k in range(8)]
    b_chip = [number(partner(k, False)) for k in range(8)]
    c_me = a_chip[0][1]
    b_me = rank(place, False)
    lo = pl.multiple_of(core * ROWS, ROWS)

    def plan(src, dst, ssem, rsem, blk, chip):
        return pltpu.make_async_remote_copy(
            src_ref=src, dst_ref=dst, send_sem=ssem, recv_sem=rsem, device_id=(blk, chip), device_id_type=MESH
        )

    def send(*where):
        plan(*where).start()

    def drain(ref, sem):
        pltpu.make_async_copy(ref, ref, sem).wait()

    barrier = pltpu.get_barrier_semaphore()

    def tell(sem, blk, chip):
        pl.semaphore_signal(sem, inc=1, device_id=(blk, chip), device_id_type=MESH)

    for d in range(3):
        tell(barrier, core, a_chip[1 << d][0])
        tell(barrier, core, b_chip[1 << d])
    tell(barrier, other, dp)

    load_q = pltpu.make_async_copy(q_hbm, q_in, in_sem.at[0])
    load_v = pltpu.make_async_copy(v_hbm, v_in, in_sem.at[1])
    load_q.start()
    load_v.start()
    load_q.wait()
    load_v.wait()

    def unit_rows(value):
        wide = value.astype(F32)
        length = jnp.sqrt(jnp.sum(wide * wide, axis=1, keepdims=True) + TINY)
        return wide / length, length

    qu, ql = unit_rows(q_in[...])
    vu, vl = unit_rows(v_in[...])
    q_hat, v_hat = qu.astype(BF16), vu.astype(BF16)
    q_unit[...] = qu
    v_unit[...] = vu
    lens[0] = ql
    lens[1] = vl
    q_own = qbuf.at[c_me, pl.ds(lo, ROWS)]
    qbuf[c_me, pl.ds(lo, ROWS), :] = q_hat
    vbuf[0] = v_hat
    hits = jnp.sum(q_hat.astype(F32) * v_hat.astype(F32), axis=0, keepdims=True)
    ybuf[core * 8 + c_me] = hits[:, :ROWS] + hits[:, ROWS:]

    pl.semaphore_wait(barrier, 7)
    for d in range(3):
        tell(near_sem.at[0], core, a_chip[1 << d][0])
        tell(near_sem.at[1], core, b_chip[1 << d])

    def gather_q(k):
        send(q_own, q_own, q_send, q_recv.at[k - 1], core, a_chip[k][0])

    def gather_v(k):
        send(vbuf.at[0], vbuf.at[SLOT[k]], v_send, v_recv.at[V_WAVE[k]], core, b_chip[k])

    send(q_own, q_own, f_send, f_recv.at[0], other, dp)
    for k in (1, 2, 4):
        gather_v(k)
        gather_q(k)
    pl.semaphore_wait(near_sem.at[0], 3)
    tell(far_sem.at[0], core, a_chip[1][0])
    for k in (3, 5, 6):
        gather_q(k)
    pl.semaphore_wait(near_sem.at[1], 3)
    tell(far_sem.at[1], core, b_chip[1])
    for k in (3, 5, 6):
        gather_v(k)
    pl.semaphore_wait(far_sem.at[0], 1)
    gather_q(7)
    pl.semaphore_wait(far_sem.at[1], 1)
    gather_v(7)
    tell(side_sem, other, dp)
    pl.semaphore_wait(side_sem, 1)
    send(q_own, q_own, f_send, f_recv.at[1], other, a_chip[7][0])

    def pass_on(ks):
        for k in ks:
            theirs = qbuf.at[a_chip[k][1], pl.ds(lo, ROWS)]
            drain(theirs, q_recv.at[k - 1])
            send(theirs, theirs, f_send, f_recv.at[0 if k in NEAR else 1], other, dp)

    def weigh(part, first, last, ks):
        rows = slice(first * ROWS, last * ROWS)
        v_part = vbuf[first:last].reshape((last - first) * ROWS, D)
        for k in ks:
            c = a_chip[k][1]
            logits = lax.dot_general(v_part, qbuf[c], (((1,), (1,)), ((), ())), preferred_element_type=F32)
            e = jnp.exp(logits * INV_TEMP)
            spart[part, c, 0:1, :] = jnp.sum(e, axis=0, keepdims=True)
            t_ref[c, rows, :] = e.astype(BF16)

    pass_on(NEAR[1:])
    drain(vbuf.at[1:4], v_recv.at[0])
    drain(qbuf.at[0:2], f_recv.at[0])
    weigh(0, 0, 4, NEAR)
    pass_on(FAR[:3])
    drain(vbuf.at[0], q_recv.at[6])
    drain(qbuf.at[0:2], f_recv.at[1])
    weigh(0, 0, 4, FAR)
    drain(vbuf.at[4:7], v_recv.at[1])
    weigh(1, 4, 7, range(8))
    drain(vbuf.at[7], v_recv.at[2])
    weigh(2, 7, 8, range(8))
    a_me = core * 8 + c_me
    for c in range(8):
        sbuf[a_me, c : c + 1, :] = spart[0, c, 0:1, :] + spart[1, c, 0:1, :] + spart[2, c, 0:1, :]
    v_all = vbuf[...].reshape(8 * ROWS, D)

    def exchange(ref, ssem, rsem):
        for k in ORDER:
            for blk in (core, other):
                send(ref, ref, ssem, rsem, blk, a_chip[k][0])
        send(ref, ref, ssem, rsem, other, dp)

    exchange(sbuf.at[a_me], s_send, s_recv)
    exchange(ybuf.at[a_me], y_send, y_recv)

    for c in range(8):
        ut = lax.dot_general(v_all, t_ref[c], (((0,), (0,)), ((), ())), preferred_element_type=F32)
        ub[0, c] = ut[:, :ROWS].astype(BF16)
        ub[1, c] = ut[:, ROWS:].astype(BF16)
    send(ub.at[other], ud, d_send, d_recv, other, dp)

    drain(ud, d_recv)
    for c in range(8):
        us[c] = (ub[core, c].astype(F32) + ud[c].astype(F32)).astype(BF16)
    for k in ORDER:
        send(us.at[a_chip[k][1]], ur.at[k], u_send, u_recv, core, a_chip[k][0])

    drain(sbuf.at[0:15], s_recv)
    total = sbuf[0]
    for a in range(1, 16):
        total = total + sbuf[a]
    inverse = 1.0 / total

    def loss_rows():
        drain(ybuf.at[0:15], y_recv)
        hits = ybuf[0]
        for a in range(1, 16):
            hits = hits + ybuf[a]
        logs = jnp.sum(jnp.log(total), axis=0, keepdims=True)
        xbuf[b_me] = (logs[:, :ROWS] + logs[:, ROWS:]) - hits * INV_TEMP
        for k in ORDER:
            send(xbuf.at[b_me], xbuf.at[b_me], x_send, x_recv, core, b_chip[k])

    def w_chunk(quarter):
        rows = slice(quarter * 256, quarter * 256 + 256)
        acc = jnp.zeros((256, D), F32)
        for c in range(8):
            probs = (t_ref[c, rows, :].astype(F32) * inverse[c : c + 1, :]).astype(BF16)
            acc = acc + jnp.dot(probs, qbuf[c], preferred_element_type=F32)
        for j in (1, 0):
            k = SLOT[quarter * 2 + j]
            part = acc[j * ROWS : (j + 1) * ROWS]
            if k == 0:
                w_own[...] = part
            else:
                wb[k] = part.astype(BF16)
                send(wb.at[k], wr.at[k], w_send, w_recv, core, b_chip[k])

    for quarter in (3, 2, 1, 0):
        w_chunk(quarter)
        if quarter == 3:
            loss_rows()

    mine = lax.broadcasted_iota(jnp.int32, total.shape, 0) == c_me
    s_row = jnp.sum(jnp.where(mine, total, 0.0), axis=0, keepdims=True)
    s_row = jnp.where(core == 0, s_row[:, :ROWS], s_row[:, ROWS:])

    def slope(pull, unit, length):
        along = jnp.sum(unit * pull, axis=1, keepdims=True)
        return (pull - unit * along) / length

    drain(ur.at[1:8], u_recv)
    u_sum = ub[core, c_me].astype(F32) + ud[c_me].astype(F32)
    for k in range(1, 8):
        u_sum = u_sum + ur[k].astype(F32)
    q_pull = (jnp.transpose(u_sum / s_row) - vbuf[0].astype(F32)) * INV_TEMP
    qs_ref[...] = slope(q_pull, q_unit[...], lens[0])

    drain(xbuf.at[0:7], x_recv)
    x_sum = xbuf[0]
    for b in range(1, 8):
        x_sum = x_sum + xbuf[b]
    hits_ref[...] = x_sum

    sent = (
        (vbuf.at[0:7], q_send),
        (qbuf.at[0:4], f_send),
        (vbuf.at[0:7], v_send),
        (sbuf.at[0:15], s_send),
        (ybuf.at[0:15], y_send),
        (ud, d_send),
        (ur.at[1:8], u_send),
        (xbuf.at[0:7], x_send),
        (wr.at[1:8], w_send),
    )
    for ref, sem in sent:
        drain(ref, sem)

    drain(wr.at[1:8], w_recv)
    w_sum = w_own[...]
    for k in range(1, 8):
        w_sum = w_sum + wr[k].astype(F32)
    v_pull = (w_sum - qbuf[c_me, pl.ds(lo, ROWS), :].astype(F32)) * INV_TEMP
    cs_ref[...] = slope(v_pull, v_unit[...], lens[1])


def write_out(l_ref, q_ref, v_ref, l_out, q_out, v_out, l_own, sem):
    q_copy = pltpu.make_async_copy(q_ref, q_out, sem.at[0])
    v_copy = pltpu.make_async_copy(v_ref, v_out, sem.at[1])
    q_copy.start()
    v_copy.start()
    l_own[0, 0] = jnp.sum(l_ref[...]) / BATCH
    l_copy = pltpu.make_async_copy(l_own, l_out, sem.at[2])
    l_copy.start()
    l_copy.wait()
    q_copy.wait()
    v_copy.wait()


def per_device(queries, items):
    dma = pltpu.SemaphoreType.DMA
    vmem = pltpu.VMEM
    parts = pl.pallas_call(
        kernel,
        out_shape=(vmem((1, ROWS), F32), vmem((ROWS, D), F32), vmem((ROWS, D), F32)),
        in_specs=[pl.BlockSpec(memory_space=pltpu.HBM)] * 2,
        out_specs=(pl.BlockSpec(memory_space=vmem),) * 3,
        scratch_shapes=[
            vmem((ROWS, D), BF16),
            vmem((ROWS, D), BF16),
            vmem((ROWS, D), F32),
            vmem((ROWS, D), F32),
            vmem((2, ROWS, 1), F32),
            vmem((8, 2 * ROWS, D), BF16),
            vmem((8, ROWS, D), BF16),
            vmem((8, 8 * ROWS, 2 * ROWS), BF16),
            vmem((16, 8, 2 * ROWS), F32),
            vmem((3, 8, 8, 2 * ROWS), F32),
            vmem((2, 8, D, ROWS), BF16),
            vmem((8, D, ROWS), BF16),
            vmem((8, D, ROWS), BF16),
            vmem((8, D, ROWS), BF16),
            vmem((8, ROWS, D), BF16),
            vmem((ROWS, D), F32),
            vmem((8, ROWS, D), BF16),
            vmem((8, 1, ROWS), F32),
            vmem((16, 1, ROWS), F32),
            dma((2,)),
            dma,
            dma((7,)),
            dma,
            dma((2,)),
            dma,
            dma((3,)),
            dma,
            dma,
            dma,
            dma,
            dma,
            dma,
            dma,
            dma,
            dma,
            dma,
            dma,
            dma,
            pltpu.SemaphoreType.REGULAR((2,)),
            pltpu.SemaphoreType.REGULAR((2,)),
            pltpu.SemaphoreType.REGULAR,
        ],
        compiler_params=pltpu.CompilerParams(collective_id=0, has_side_effects=True),
    )(queries, items)
    loss, q_slope, v_slope = pl.pallas_call(
        write_out,
        out_shape=(
            jax.ShapeDtypeStruct((1, 1), F32),
            jax.ShapeDtypeStruct((ROWS, D), F32),
            jax.ShapeDtypeStruct((ROWS, D), F32),
        ),
        in_specs=[pl.BlockSpec(memory_space=vmem)] * 3,
        out_specs=(
            pl.BlockSpec(memory_space=pltpu.HBM),
            pl.BlockSpec(memory_space=pltpu.HBM),
            pl.BlockSpec(memory_space=pltpu.HBM),
        ),
        scratch_shapes=[pltpu.SMEM((1, 1), F32), dma((3,))],
        compiler_params=pltpu.CompilerParams(vmem_limit_bytes=1024 * 1024),
    )(*(pltpu.with_memory_space_constraint(part, vmem) for part in parts))
    return loss.reshape(()), q_slope, v_slope


def solution(mesh):
    spec = P(("blk", "dp"), None)
    return jax.shard_map(
        per_device, mesh=mesh, in_specs=(spec, spec), out_specs=(P(), spec, spec), check_vma=False
    )
```

```python
import jax
import jax.numpy as jnp
from jax import lax
from jax.experimental import pallas as pl
from jax.experimental.pallas import tpu as pltpu
from jax.sharding import PartitionSpec as P

MESH = pl.DeviceIdType.MESH
ROWS = 128
D = 256
BATCH = 16384
INV_TEMP = 20.0
TINY = 1e-12
F32 = jnp.float32
BF16 = jnp.bfloat16
A_LOW = (True, True, True)
SLOT = (0, 1, 2, 4, 3, 5, 6, 7)
NEAR, FAR = (0, 1, 2, 4), (3, 5, 6, 7)
WAVE = (None, 0, 0, 1, 0, 1, 1, 2)
W_ORDER = ((7, 6), (5, 3), (4, 2), (1, 0))
ORDER = (7, 3, 5, 6, 1, 2, 4)


def flip_low(p, d):
    return p + 1 - 2 * lax.rem(p, 2) if d else p


def flip_high(p, d):
    return 3 - p if d else p


def low_bit(p):
    return lax.rem(lax.div(p + 1, 2), 2)


def high_bit(p):
    return lax.div(p, 2)


def kernel(
    q_hbm,
    v_hbm,
    hits_ref,
    qs_ref,
    cs_ref,
    given,
    q_unit,
    v_unit,
    lens,
    qbuf,
    vbuf,
    t_ref,
    sbuf,
    spart,
    ub,
    ud,
    us,
    ur,
    wb,
    w_own,
    wr,
    xbuf,
    ybuf,
    in_sem,
    q_recv,
    f_recv,
    v_recv,
    big_send,
    small_send,
    s_send,
    s_recv,
    d_recv,
    u_recv,
    w_recv,
    x_recv,
    y_recv,
    near_sem,
    far_sem,
):
    core = lax.axis_index("blk")
    other = 1 - core
    dp = lax.axis_index("dp")
    z, y, x = lax.div(dp, 16), lax.rem(lax.div(dp, 4), 4), lax.rem(dp, 4)

    place = (z, y, x)

    def partner(k, low):
        steps = ((k >> 2) & 1, (k >> 1) & 1, k & 1)
        zz, yy, xx = (
            (flip_low if is_low == low else flip_high)(p, d) for p, d, is_low in zip(place, steps, A_LOW)
        )
        return zz, yy, xx

    def rank(place, low):
        bits = [(low_bit if is_low == low else high_bit)(p) for p, is_low in zip(place, A_LOW)]
        return bits[0] * 4 + bits[1] * 2 + bits[2]

    def number(place):
        return place[0] * 16 + place[1] * 4 + place[2]

    a_chip = [(number(partner(k, True)), rank(partner(k, True), True)) for k in range(8)]
    b_chip = [number(partner(k, False)) for k in range(8)]
    c_me = a_chip[0][1]
    b_me = rank(place, False)
    lo = pl.multiple_of(core * ROWS, ROWS)

    def plan(src, dst, ssem, rsem, blk, chip):
        return pltpu.make_async_remote_copy(
            src_ref=src, dst_ref=dst, send_sem=ssem, recv_sem=rsem, device_id=(blk, chip), device_id_type=MESH
        )

    def send(*where):
        plan(*where).start()

    def drain(ref, sem):
        pltpu.make_async_copy(ref, ref, sem).wait()

    barrier = pltpu.get_barrier_semaphore()

    def tell(sem, blk, chip):
        pl.semaphore_signal(sem, inc=1, device_id=(blk, chip), device_id_type=MESH)

    for d in range(3):
        tell(barrier, core, a_chip[1 << d][0])
        tell(barrier, core, b_chip[1 << d])
    tell(barrier, other, dp)

    pltpu.make_async_copy(q_hbm, given.at[0], in_sem).start()
    pltpu.make_async_copy(v_hbm, given.at[1], in_sem).start()
    drain(given, in_sem)

    def unit_rows(value):
        wide = value.astype(F32)
        length = jnp.sqrt(jnp.sum(wide * wide, axis=1, keepdims=True) + TINY)
        return wide / length, length

    qu, ql = unit_rows(given[0])
    vu, vl = unit_rows(given[1])
    q_hat, v_hat = qu.astype(BF16), vu.astype(BF16)
    q_unit[...] = qu
    v_unit[...] = vu
    lens[0] = ql
    lens[1] = vl
    q_own = qbuf.at[c_me, pl.ds(lo, ROWS)]
    qbuf[c_me, pl.ds(lo, ROWS), :] = q_hat
    vbuf[0] = v_hat
    hits = jnp.sum(q_hat.astype(F32) * v_hat.astype(F32), axis=0, keepdims=True)
    ybuf[core * 8 + c_me] = hits[:, :ROWS] + hits[:, ROWS:]

    pl.semaphore_wait(barrier, 7)
    for d in range(3):
        tell(near_sem.at[0], core, a_chip[1 << d][0])
        tell(near_sem.at[1], core, b_chip[1 << d])

    def gather_q(k):
        send(q_own, q_own, big_send, q_recv.at[WAVE[k]], core, a_chip[k][0])

    def gather_v(k):
        send(vbuf.at[0], vbuf.at[SLOT[k]], big_send, v_recv.at[WAVE[k]], core, b_chip[k])

    send(q_own, q_own, big_send, f_recv.at[0], other, dp)
    for k in (1, 2, 4):
        gather_v(k)
        gather_q(k)
    pl.semaphore_wait(near_sem.at[0], 3)
    tell(far_sem.at[0], core, a_chip[1][0])
    for k in (3, 5, 6):
        gather_q(k)
    pl.semaphore_wait(near_sem.at[1], 3)
    tell(far_sem.at[1], core, b_chip[1])
    for k in (3, 5, 6):
        gather_v(k)
    pl.semaphore_wait(far_sem.at[0], 1)
    gather_q(7)
    pl.semaphore_wait(far_sem.at[1], 1)
    gather_v(7)
    def pass_on(ks):
        drain(vbuf.at[0 : len(ks)], q_recv.at[WAVE[ks[0]]])
        for k in ks:
            theirs = qbuf.at[a_chip[k][1], pl.ds(lo, ROWS)]
            send(theirs, theirs, big_send, f_recv.at[0 if k in NEAR else 1], other, dp)

    def weigh(part, first, last, ks):
        rows = slice(first * ROWS, last * ROWS)
        v_part = vbuf[first:last].reshape((last - first) * ROWS, D)
        for k in ks:
            c = a_chip[k][1]
            logits = lax.dot_general(v_part, qbuf[c], (((1,), (1,)), ((), ())), preferred_element_type=F32)
            e = jnp.exp(logits * INV_TEMP)
            spart[part, c, 0:1, :] = jnp.sum(e, axis=0, keepdims=True)
            t_ref[c, rows, :] = e.astype(BF16)

    pass_on(NEAR[1:])
    drain(vbuf.at[1:4], v_recv.at[0])
    drain(qbuf.at[0:2], f_recv.at[0])
    pass_on(FAR[:3])
    weigh(0, 0, 4, NEAR)
    pass_on(FAR[3:])
    drain(qbuf.at[0:2], f_recv.at[1])
    weigh(0, 0, 4, FAR)
    drain(vbuf.at[4:7], v_recv.at[1])
    weigh(1, 4, 7, range(8))
    drain(vbuf.at[7], v_recv.at[2])
    weigh(2, 7, 8, range(8))
    a_me = core * 8 + c_me
    for c in range(8):
        sbuf[a_me, c : c + 1, :] = spart[0, c, 0:1, :] + spart[1, c, 0:1, :] + spart[2, c, 0:1, :]
    v_all = vbuf[...].reshape(8 * ROWS, D)

    def exchange(ref, ssem, rsem):
        for k in ORDER:
            for blk in (core, other):
                send(ref, ref, ssem, rsem, blk, a_chip[k][0])
        send(ref, ref, ssem, rsem, other, dp)

    exchange(sbuf.at[a_me], s_send, s_recv)
    exchange(ybuf.at[a_me], small_send, y_recv)

    for c in range(8):
        ut = lax.dot_general(v_all, t_ref[c], (((0,), (0,)), ((), ())), preferred_element_type=F32)
        ub[0, c] = ut[:, :ROWS].astype(BF16)
        ub[1, c] = ut[:, ROWS:].astype(BF16)
    send(ub.at[other], ud, big_send, d_recv, other, dp)

    drain(ud, d_recv)
    for c in range(8):
        us[c] = (ub[core, c].astype(F32) + ud[c].astype(F32)).astype(BF16)
    for k in ORDER:
        send(us.at[a_chip[k][1]], ur.at[k], big_send, u_recv, core, a_chip[k][0])

    drain(sbuf.at[0:15], s_recv)
    total = sbuf[0]
    for a in range(1, 16):
        total = total + sbuf[a]
    inverse = 1.0 / total
    scales = [jnp.broadcast_to(inverse[c : c + 1, :], (1, 16, 2 * ROWS)).astype(BF16) for c in range(8)]

    def loss_rows():
        drain(ybuf.at[0:15], y_recv)
        hits = ybuf[0]
        for a in range(1, 16):
            hits = hits + ybuf[a]
        logs = jnp.sum(jnp.log(total), axis=0, keepdims=True)
        xbuf[b_me] = (logs[:, :ROWS] + logs[:, ROWS:]) - hits * INV_TEMP
        for k in ORDER:
            send(xbuf.at[b_me], xbuf.at[b_me], small_send, x_recv, core, b_chip[k])

    def pull_items(ks):
        acc = jnp.zeros((2 * ROWS, D), F32)
        for c in range(8):
            rows = [t_ref[c, SLOT[k] * ROWS : (SLOT[k] + 1) * ROWS, :] for k in ks]
            probs = jnp.concatenate(rows).reshape(16, 16, 2 * ROWS) * scales[c]
            acc = acc + jnp.dot(probs.reshape(2 * ROWS, 2 * ROWS), qbuf[c], preferred_element_type=F32)
        for k, part in zip(ks, (acc[:ROWS], acc[ROWS:])):
            if k == 0:
                w_own[...] = part
            else:
                wb[k] = part.astype(BF16)
                send(wb.at[k], wr.at[k], big_send, w_recv, core, b_chip[k])

    for n, ks in enumerate(W_ORDER):
        pull_items(ks)
        if n == 0:
            loss_rows()

    mine = lax.broadcasted_iota(jnp.int32, total.shape, 0) == c_me
    s_row = jnp.sum(jnp.where(mine, total, 0.0), axis=0, keepdims=True)
    s_row = jnp.where(core == 0, s_row[:, :ROWS], s_row[:, ROWS:])

    def slope(pull, unit, length):
        along = jnp.sum(unit * pull, axis=1, keepdims=True)
        return (pull - unit * along) / length

    drain(ur.at[1:8], u_recv)
    u_sum = ub[core, c_me].astype(F32) + ud[c_me].astype(F32)
    for k in range(1, 8):
        u_sum = u_sum + ur[k].astype(F32)
    q_pull = (jnp.transpose(u_sum / s_row) - vbuf[0].astype(F32)) * INV_TEMP
    qs_ref[...] = slope(q_pull, q_unit[...], lens[0])

    drain(xbuf.at[0:7], x_recv)
    x_sum = xbuf[0]
    for b in range(1, 8):
        x_sum = x_sum + xbuf[b]
    hits_ref[...] = x_sum

    drain(t_ref.at[:, 0:704, :], big_send)
    drain(sbuf.at[0:15], s_send)
    drain(ybuf.at[0:22], small_send)

    drain(wr.at[1:8], w_recv)
    w_sum = w_own[...]
    for k in range(1, 8):
        w_sum = w_sum + wr[k].astype(F32)
    v_pull = (w_sum - qbuf[c_me, pl.ds(lo, ROWS), :].astype(F32)) * INV_TEMP
    cs_ref[...] = slope(v_pull, v_unit[...], lens[1])


def write_out(l_ref, q_ref, v_ref, l_out, q_out, v_out, l_own, sem):
    q_copy = pltpu.make_async_copy(q_ref, q_out, sem.at[0])
    v_copy = pltpu.make_async_copy(v_ref, v_out, sem.at[1])
    q_copy.start()
    v_copy.start()
    l_own[0, 0] = jnp.sum(l_ref[...]) / BATCH
    l_copy = pltpu.make_async_copy(l_own, l_out, sem.at[2])
    l_copy.start()
    l_copy.wait()
    q_copy.wait()
    v_copy.wait()


def per_device(queries, items):
    dma = pltpu.SemaphoreType.DMA
    vmem = pltpu.VMEM
    parts = pl.pallas_call(
        kernel,
        out_shape=(vmem((1, ROWS), F32), vmem((ROWS, D), F32), vmem((ROWS, D), F32)),
        in_specs=[pl.BlockSpec(memory_space=pltpu.HBM)] * 2,
        out_specs=(pl.BlockSpec(memory_space=vmem),) * 3,
        scratch_shapes=[
            vmem((2, ROWS, D), BF16),
            vmem((ROWS, D), F32),
            vmem((ROWS, D), F32),
            vmem((2, ROWS, 1), F32),
            vmem((8, 2 * ROWS, D), BF16),
            vmem((8, ROWS, D), BF16),
            vmem((8, 8 * ROWS, 2 * ROWS), BF16),
            vmem((16, 8, 2 * ROWS), F32),
            vmem((3, 8, 8, 2 * ROWS), F32),
            vmem((2, 8, D, ROWS), BF16),
            vmem((8, D, ROWS), BF16),
            vmem((8, D, ROWS), BF16),
            vmem((8, D, ROWS), BF16),
            vmem((8, ROWS, D), BF16),
            vmem((ROWS, D), F32),
            vmem((8, ROWS, D), BF16),
            vmem((8, 1, ROWS), F32),
            vmem((24, 1, ROWS), F32),
            dma,
            dma((3,)),
            dma((2,)),
            dma((3,)),
            dma,
            dma,
            dma,
            dma,
            dma,
            dma,
            dma,
            dma,
            dma,
            pltpu.SemaphoreType.REGULAR((2,)),
            pltpu.SemaphoreType.REGULAR((2,)),
        ],
        compiler_params=pltpu.CompilerParams(collective_id=0, has_side_effects=True),
    )(queries, items)
    loss, q_slope, v_slope = pl.pallas_call(
        write_out,
        out_shape=(
            jax.ShapeDtypeStruct((1, 1), F32),
            jax.ShapeDtypeStruct((ROWS, D), F32),
            jax.ShapeDtypeStruct((ROWS, D), F32),
        ),
        in_specs=[pl.BlockSpec(memory_space=vmem)] * 3,
        out_specs=(
            pl.BlockSpec(memory_space=pltpu.HBM),
            pl.BlockSpec(memory_space=pltpu.HBM),
            pl.BlockSpec(memory_space=pltpu.HBM),
        ),
        scratch_shapes=[pltpu.SMEM((1, 1), F32), dma((3,))],
        compiler_params=pltpu.CompilerParams(vmem_limit_bytes=1024 * 1024),
    )(*(pltpu.with_memory_space_constraint(part, vmem) for part in parts))
    return loss.reshape(()), q_slope, v_slope


def solution(mesh):
    spec = P(("blk", "dp"), None)
    return jax.shard_map(
        per_device, mesh=mesh, in_specs=(spec, spec), out_specs=(P(), spec, spec), check_vma=False
    )
```

```python
import functools

import jax
import jax.numpy as jnp
from jax import lax
from jax.experimental import pallas as pl
from jax.experimental.pallas import tpu as pltpu
from jax.sharding import PartitionSpec as P

MESH = pl.DeviceIdType.MESH
ROWS = 128
D = 256
BATCH = 16384
INV_TEMP = 20.0
TINY = 1e-12
F32 = jnp.float32
BF16 = jnp.bfloat16
A_LOW = (True, False, True)
SLOT = (0, 1, 2, 4, 3, 5, 6, 7)
NEAR, FAR = (0, 1, 2, 4), (3, 5, 6, 7)
WAVE = (None, 0, 0, 1, 0, 1, 1, 2)
W_ORDER = ((0,), (2, 1), (3, 4), (6, 5), (7,))
ORDER = (7, 3, 5, 6, 1, 2, 4)


def flip_low(p, d):
    return p + 1 - 2 * lax.rem(p, 2) if d else p


def flip_high(p, d):
    return 3 - p if d else p


def low_bit(p):
    return lax.rem(lax.div(p + 1, 2), 2)


def high_bit(p):
    return lax.div(p, 2)


def kernel(
    q_hbm,
    v_hbm,
    hits_ref,
    qs_ref,
    cs_ref,
    given,
    q_unit,
    v_unit,
    lens,
    qbuf,
    vbuf,
    t_ref,
    sbuf,
    spart,
    ub,
    ud,
    us,
    ur,
    wb,
    w_own,
    wr,
    xbuf,
    ybuf,
    in_sem,
    q_recv,
    f_recv,
    v_recv,
    big_send,
    small_send,
    s_send,
    s_recv,
    d_recv,
    u_recv,
    w_recv,
    x_recv,
    y_recv,
    near_sem,
    far_sem,
):
    core = lax.axis_index("blk")
    other = 1 - core
    dp = lax.axis_index("dp")
    z, y, x = lax.div(dp, 16), lax.rem(lax.div(dp, 4), 4), lax.rem(dp, 4)

    place = (z, y, x)

    def partner(k, low):
        steps = ((k >> 2) & 1, (k >> 1) & 1, k & 1)
        zz, yy, xx = (
            (flip_low if is_low == low else flip_high)(p, d) for p, d, is_low in zip(place, steps, A_LOW)
        )
        return zz, yy, xx

    def rank(place, low):
        bits = [(low_bit if is_low == low else high_bit)(p) for p, is_low in zip(place, A_LOW)]
        return bits[0] * 4 + bits[1] * 2 + bits[2]

    def number(place):
        return place[0] * 16 + place[1] * 4 + place[2]

    a_chip = [(number(partner(k, True)), rank(partner(k, True), True)) for k in range(8)]
    b_chip = [number(partner(k, False)) for k in range(8)]
    c_me = a_chip[0][1]
    b_me = rank(place, False)

    b_bits = [high_bit(p) if is_low else low_bit(p) for p, is_low in zip(place, A_LOW)]
    lo = pl.multiple_of(core * ROWS, ROWS)

    def plan(src, dst, ssem, rsem, blk, chip):
        return pltpu.make_async_remote_copy(
            src_ref=src, dst_ref=dst, send_sem=ssem, recv_sem=rsem, device_id=(blk, chip), device_id_type=MESH
        )

    def send(*where):
        plan(*where).start()

    def drain(ref, sem):
        pltpu.make_async_copy(ref, ref, sem).wait()

    barrier = pltpu.get_barrier_semaphore()

    def tell(sem, blk, chip):
        pl.semaphore_signal(sem, inc=1, device_id=(blk, chip), device_id_type=MESH)

    for d in range(3):
        tell(barrier, core, a_chip[1 << d][0])
        tell(barrier, core, b_chip[1 << d])
    tell(barrier, other, dp)

    pltpu.make_async_copy(q_hbm, given.at[0], in_sem).start()
    pltpu.make_async_copy(v_hbm, given.at[1], in_sem).start()
    drain(given, in_sem)

    def unit_rows(value):
        wide = value.astype(F32)
        length = jnp.sqrt(jnp.sum(wide * wide, axis=1, keepdims=True) + TINY)
        return wide / length, length

    qu, ql = unit_rows(given[0])
    vu, vl = unit_rows(given[1])
    q_hat, v_hat = qu.astype(BF16), vu.astype(BF16)
    q_unit[...] = qu
    v_unit[...] = vu
    lens[0] = ql
    lens[1] = vl
    q_own = qbuf.at[c_me, pl.ds(lo, ROWS)]
    qbuf[c_me, pl.ds(lo, ROWS), :] = q_hat
    vbuf[0] = v_hat
    hits = jnp.sum(q_hat.astype(F32) * v_hat.astype(F32), axis=0, keepdims=True)
    ybuf[core * 8 + c_me] = hits[:, :ROWS] + hits[:, ROWS:]

    pl.semaphore_wait(barrier, 7)
    for d in range(3):
        tell(near_sem.at[0], core, a_chip[1 << d][0])
        tell(near_sem.at[1], core, b_chip[1 << d])

    def gather_q(k):
        send(q_own, q_own, big_send, q_recv.at[WAVE[k]], core, a_chip[k][0])

    def gather_v(k):
        send(vbuf.at[0], vbuf.at[SLOT[k]], big_send, v_recv.at[WAVE[k]], core, b_chip[k])

    send(q_own, q_own, big_send, f_recv.at[0], other, dp)
    for k in (1, 2, 4):
        gather_v(k)
        gather_q(k)
    pl.semaphore_wait(near_sem.at[0], 3)
    tell(far_sem.at[0], core, a_chip[1][0])
    for k in (3, 5, 6):
        gather_q(k)
    pl.semaphore_wait(near_sem.at[1], 3)
    tell(far_sem.at[1], core, b_chip[1])
    for k in (3, 5, 6):
        gather_v(k)
    pl.semaphore_wait(far_sem.at[0], 1)
    gather_q(7)
    pl.semaphore_wait(far_sem.at[1], 1)
    gather_v(7)
    def pass_on(ks):
        drain(vbuf.at[0 : len(ks)], q_recv.at[WAVE[ks[0]]])
        for k in ks:
            theirs = qbuf.at[a_chip[k][1], pl.ds(lo, ROWS)]
            send(theirs, theirs, big_send, f_recv.at[0 if k in NEAR else 1], other, dp)

    def weigh(part, first, last, ks):
        rows = slice(first * ROWS, last * ROWS)
        v_part = vbuf[first:last].reshape((last - first) * ROWS, D)
        for k in ks:
            c = a_chip[k][1]
            logits = lax.dot_general(v_part, qbuf[c], (((1,), (1,)), ((), ())), preferred_element_type=F32)
            e = jnp.exp(logits * INV_TEMP)
            spart[part, c, 0:1, :] = jnp.sum(e, axis=0, keepdims=True)
            t_ref[c, rows, :] = e.astype(BF16)

    pass_on(NEAR[1:])
    drain(vbuf.at[1:4], v_recv.at[0])
    drain(qbuf.at[0:2], f_recv.at[0])
    pass_on(FAR[:3])
    weigh(0, 0, 4, NEAR)
    pass_on(FAR[3:])
    drain(qbuf.at[0:2], f_recv.at[1])
    weigh(0, 0, 4, FAR)
    drain(vbuf.at[4:7], v_recv.at[1])
    weigh(1, 4, 7, range(8))
    drain(vbuf.at[7], v_recv.at[2])
    weigh(2, 7, 8, range(8))
    a_me = core * 8 + c_me
    for c in range(8):
        sbuf[a_me, c : c + 1, :] = spart[0, c, 0:1, :] + spart[1, c, 0:1, :] + spart[2, c, 0:1, :]
    v_all = vbuf[...].reshape(8 * ROWS, D)

    def exchange(ref, ssem, rsem):
        for k in ORDER:
            for blk in (core, other):
                send(ref, ref, ssem, rsem, blk, a_chip[k][0])
        send(ref, ref, ssem, rsem, other, dp)

    exchange(sbuf.at[a_me], s_send, s_recv)
    exchange(ybuf.at[a_me], small_send, y_recv)

    for c in range(8):
        ut = lax.dot_general(v_all, t_ref[c], (((0,), (0,)), ((), ())), preferred_element_type=F32)
        ub[0, c] = ut[:, :ROWS].astype(BF16)
        ub[1, c] = ut[:, ROWS:].astype(BF16)
    send(ub.at[other], ud, big_send, d_recv, other, dp)

    drain(ud, d_recv)
    for c in range(8):
        us[c] = (ub[core, c].astype(F32) + ud[c].astype(F32)).astype(BF16)
    for k in ORDER:
        send(us.at[a_chip[k][1]], ur.at[k], big_send, u_recv, core, a_chip[k][0])

    drain(sbuf.at[0:15], s_recv)
    total = sbuf[0]
    for a in range(1, 16):
        total = total + sbuf[a]
    inverse = 1.0 / total
    scales = [jnp.broadcast_to(inverse[c : c + 1, :], (1, 16, 2 * ROWS)).astype(BF16) for c in range(8)]

    def loss_rows():
        drain(ybuf.at[0:15], y_recv)
        hits = ybuf[0]
        for a in range(1, 16):
            hits = hits + ybuf[a]
        logs = jnp.sum(jnp.log(total), axis=0, keepdims=True)
        xbuf[b_me] = (logs[:, :ROWS] + logs[:, ROWS:]) - hits * INV_TEMP
        for k in ORDER:
            send(xbuf.at[b_me], xbuf.at[b_me], small_send, x_recv, core, b_chip[k])

    def pull(rows, n):
        acc = jnp.zeros((n, D), F32)
        for c in range(8):
            probs = rows(c).reshape(n // 16, 16, 2 * ROWS) * scales[c]
            acc = acc + jnp.dot(probs.reshape(n, 2 * ROWS), qbuf[c], preferred_element_type=F32)
        return acc

    def give(k, part, chip):
        wb[k] = part.astype(BF16)
        send(wb.at[k], wr.at[k], big_send, w_recv, core, chip)

    def keep(part):
        w_own[...] = part

    for n, targets in enumerate(W_ORDER):
        ks, rows, chips = [], [], []
        for b in targets:
            bits = ((b >> 2) & 1, (b >> 1) & 1, b & 1)
            dz, dy, dx = (1 - own if bit else own for bit, own in zip(bits, b_bits))
            k = 4 * dz + 2 * dy + dx
            slot = k - dz * (1 - dy) * (1 - dx) + (1 - dz) * dy * dx
            ks.append(k)
            rows.append(pl.ds(pl.multiple_of(slot * ROWS, ROWS), ROWS))
            chips.append(
                number(
                    [
                        (3 - low_bit(p) if bit else low_bit(p)) if is_low else high_bit(p) * (3 - 2 * bit) + bit
                        for p, bit, is_low in zip(place, bits, A_LOW)
                    ]
                )
            )
        acc = pull(lambda c: jnp.concatenate([t_ref[c, r, :] for r in rows]), len(targets) * ROWS)
        for m, b in enumerate(targets):
            part = acc[m * ROWS : (m + 1) * ROWS]
            pl.when(b_me == b)(functools.partial(keep, part))
            pl.when(b_me != b)(functools.partial(give, ks[m], part, chips[m]))
        if n == 0:
            loss_rows()

    mine = lax.broadcasted_iota(jnp.int32, total.shape, 0) == c_me
    s_row = jnp.sum(jnp.where(mine, total, 0.0), axis=0, keepdims=True)
    s_row = jnp.where(core == 0, s_row[:, :ROWS], s_row[:, ROWS:])

    def slope(pull, unit, length):
        along = jnp.sum(unit * pull, axis=1, keepdims=True)
        return (pull - unit * along) / length

    drain(ur.at[1:8], u_recv)
    u_sum = ub[core, c_me].astype(F32) + ud[c_me].astype(F32)
    for k in range(1, 8):
        u_sum = u_sum + ur[k].astype(F32)
    q_pull = (jnp.transpose(u_sum / s_row) - vbuf[0].astype(F32)) * INV_TEMP
    qs_ref[...] = slope(q_pull, q_unit[...], lens[0])

    drain(xbuf.at[0:7], x_recv)
    x_sum = xbuf[0]
    for b in range(1, 8):
        x_sum = x_sum + xbuf[b]
    hits_ref[...] = x_sum

    drain(t_ref.at[:, 0:704, :], big_send)
    drain(sbuf.at[0:15], s_send)
    drain(ybuf.at[0:22], small_send)

    drain(wr.at[1:8], w_recv)
    w_sum = w_own[...]
    for k in range(1, 8):
        w_sum = w_sum + wr[k].astype(F32)
    v_pull = (w_sum - qbuf[c_me, pl.ds(lo, ROWS), :].astype(F32)) * INV_TEMP
    cs_ref[...] = slope(v_pull, v_unit[...], lens[1])


def write_out(l_ref, q_ref, v_ref, l_out, q_out, v_out, l_own, sem):
    q_copy = pltpu.make_async_copy(q_ref, q_out, sem.at[0])
    v_copy = pltpu.make_async_copy(v_ref, v_out, sem.at[1])
    q_copy.start()
    v_copy.start()
    l_own[0, 0] = jnp.sum(l_ref[...]) / BATCH
    l_copy = pltpu.make_async_copy(l_own, l_out, sem.at[2])
    l_copy.start()
    l_copy.wait()
    q_copy.wait()
    v_copy.wait()


def per_device(queries, items):
    dma = pltpu.SemaphoreType.DMA
    vmem = pltpu.VMEM
    parts = pl.pallas_call(
        kernel,
        out_shape=(vmem((1, ROWS), F32), vmem((ROWS, D), F32), vmem((ROWS, D), F32)),
        in_specs=[pl.BlockSpec(memory_space=pltpu.HBM)] * 2,
        out_specs=(pl.BlockSpec(memory_space=vmem),) * 3,
        scratch_shapes=[
            vmem((2, ROWS, D), BF16),
            vmem((ROWS, D), F32),
            vmem((ROWS, D), F32),
            vmem((2, ROWS, 1), F32),
            vmem((8, 2 * ROWS, D), BF16),
            vmem((8, ROWS, D), BF16),
            vmem((8, 8 * ROWS, 2 * ROWS), BF16),
            vmem((16, 8, 2 * ROWS), F32),
            vmem((3, 8, 8, 2 * ROWS), F32),
            vmem((2, 8, D, ROWS), BF16),
            vmem((8, D, ROWS), BF16),
            vmem((8, D, ROWS), BF16),
            vmem((8, D, ROWS), BF16),
            vmem((8, ROWS, D), BF16),
            vmem((ROWS, D), F32),
            vmem((8, ROWS, D), BF16),
            vmem((8, 1, ROWS), F32),
            vmem((24, 1, ROWS), F32),
            dma,
            dma((3,)),
            dma((2,)),
            dma((3,)),
            dma,
            dma,
            dma,
            dma,
            dma,
            dma,
            dma,
            dma,
            dma,
            pltpu.SemaphoreType.REGULAR((2,)),
            pltpu.SemaphoreType.REGULAR((2,)),
        ],
        compiler_params=pltpu.CompilerParams(collective_id=0, has_side_effects=True),
    )(queries, items)
    loss, q_slope, v_slope = pl.pallas_call(
        write_out,
        out_shape=(
            jax.ShapeDtypeStruct((1, 1), F32),
            jax.ShapeDtypeStruct((ROWS, D), F32),
            jax.ShapeDtypeStruct((ROWS, D), F32),
        ),
        in_specs=[pl.BlockSpec(memory_space=vmem)] * 3,
        out_specs=(
            pl.BlockSpec(memory_space=pltpu.HBM),
            pl.BlockSpec(memory_space=pltpu.HBM),
            pl.BlockSpec(memory_space=pltpu.HBM),
        ),
        scratch_shapes=[pltpu.SMEM((1, 1), F32), dma((3,))],
        compiler_params=pltpu.CompilerParams(vmem_limit_bytes=1024 * 1024),
    )(*(pltpu.with_memory_space_constraint(part, vmem) for part in parts))
    return loss.reshape(()), q_slope, v_slope


def solution(mesh):
    spec = P(("blk", "dp"), None)
    return jax.shard_map(
        per_device, mesh=mesh, in_specs=(spec, spec), out_specs=(P(), spec, spec), check_vma=False
    )
```

```python
import functools

import jax
import jax.numpy as jnp
from jax import lax
from jax.experimental import pallas as pl
from jax.experimental.pallas import tpu as pltpu
from jax.sharding import PartitionSpec as P

MESH = pl.DeviceIdType.MESH
ROWS = 128
D = 256
BATCH = 16384
INV_TEMP = 20.0
TINY = 1e-12
F32 = jnp.float32
BF16 = jnp.bfloat16
A_LOW = (True, False, True)
SLOT = (0, 1, 2, 4, 3, 5, 6, 7)
NEAR, FAR = (0, 1, 2, 4), (3, 5, 6, 7)
WAVE = (None, 0, 0, 1, 0, 1, 1, 2)
W_ORDER = ((0,), (2, 1), (3, 4), (6, 5), (7,))
ORDER = (7, 3, 5, 6, 1, 2, 4)


def flip_low(p, d):
    return p + 1 - 2 * (p & 1) if d else p


def flip_high(p, d):
    return 3 - p if d else p


def low_bit(p):
    return ((p + 1) >> 1) & 1


def high_bit(p):
    return p >> 1


def kernel(
    q_hbm,
    v_hbm,
    hits_ref,
    qs_ref,
    cs_ref,
    given,
    q_unit,
    v_unit,
    lens,
    qbuf,
    vbuf,
    t_ref,
    sbuf,
    spart,
    ub,
    ud,
    us,
    ur,
    wb,
    w_own,
    wr,
    xbuf,
    ybuf,
    in_sem,
    q_recv,
    f_recv,
    v_recv,
    big_send,
    small_send,
    s_send,
    s_recv,
    d_recv,
    u_recv,
    w_recv,
    x_recv,
    y_recv,
    near_sem,
    far_sem,
):
    core = lax.axis_index("blk")
    other = 1 - core
    dp = lax.axis_index("dp")
    z, y, x = dp >> 4, (dp >> 2) & 3, dp & 3

    place = (z, y, x)

    def partner(k, low):
        steps = ((k >> 2) & 1, (k >> 1) & 1, k & 1)
        zz, yy, xx = (
            (flip_low if is_low == low else flip_high)(p, d) for p, d, is_low in zip(place, steps, A_LOW)
        )
        return zz, yy, xx

    def rank(place, low):
        bits = [(low_bit if is_low == low else high_bit)(p) for p, is_low in zip(place, A_LOW)]
        return bits[0] * 4 + bits[1] * 2 + bits[2]

    def number(place):
        return place[0] * 16 + place[1] * 4 + place[2]

    a_place = {k: partner(k, True) for k in (1, 2, 4)}
    b_place = {k: partner(k, False) for k in (1, 2, 4)}
    barrier = pltpu.get_barrier_semaphore()

    def tell(sem, blk, chip):
        pl.semaphore_signal(sem, inc=1, device_id=(blk, chip), device_id_type=MESH)

    tell(barrier, other, dp)
    for k in (1, 2, 4):
        tell(barrier, core, number(b_place[k]))
        tell(barrier, core, number(a_place[k]))

    pltpu.make_async_copy(q_hbm, given.at[0], in_sem).start()
    pltpu.make_async_copy(v_hbm, given.at[1], in_sem).start()

    a_chip = [(number(partner(k, True)), rank(partner(k, True), True)) for k in range(8)]
    b_chip = [number(partner(k, False)) for k in range(8)]
    c_me = a_chip[0][1]
    b_me = rank(place, False)

    b_bits = [high_bit(p) if is_low else low_bit(p) for p, is_low in zip(place, A_LOW)]
    lo = pl.multiple_of(core * ROWS, ROWS)

    def plan(src, dst, ssem, rsem, blk, chip):
        return pltpu.make_async_remote_copy(
            src_ref=src, dst_ref=dst, send_sem=ssem, recv_sem=rsem, device_id=(blk, chip), device_id_type=MESH
        )

    def send(*where):
        plan(*where).start()

    def drain(ref, sem):
        pltpu.make_async_copy(ref, ref, sem).wait()

    drain(given, in_sem)

    def unit_rows(value):
        wide = value.astype(F32)
        length = jnp.sqrt(jnp.sum(wide * wide, axis=1, keepdims=True) + TINY)
        return wide / length, length

    qu, ql = unit_rows(given[0])
    vu, vl = unit_rows(given[1])
    q_hat, v_hat = qu.astype(BF16), vu.astype(BF16)
    q_unit[...] = qu
    v_unit[...] = vu
    lens[0] = ql
    lens[1] = vl
    q_own = qbuf.at[c_me, pl.ds(lo, ROWS)]
    qbuf[c_me, pl.ds(lo, ROWS), :] = q_hat
    vbuf[0] = v_hat
    hits = jnp.sum(q_hat.astype(F32) * v_hat.astype(F32), axis=0, keepdims=True)
    ybuf[core * 8 + c_me] = hits[:, :ROWS] + hits[:, ROWS:]

    pl.semaphore_wait(barrier, 7)
    for d in range(3):
        tell(near_sem.at[0], core, a_chip[1 << d][0])
        tell(near_sem.at[1], core, b_chip[1 << d])

    def gather_q(k):
        send(q_own, q_own, big_send, q_recv.at[WAVE[k]], core, a_chip[k][0])

    def gather_v(k):
        send(vbuf.at[0], vbuf.at[SLOT[k]], big_send, v_recv.at[WAVE[k]], core, b_chip[k])

    send(q_own, q_own, big_send, f_recv.at[0], other, dp)
    for k in (1, 2, 4):
        gather_v(k)
        gather_q(k)
    pl.semaphore_wait(near_sem.at[0], 3)
    tell(far_sem.at[0], core, a_chip[1][0])
    for k in (3, 5, 6):
        gather_q(k)
    pl.semaphore_wait(near_sem.at[1], 3)
    tell(far_sem.at[1], core, b_chip[1])
    for k in (3, 5, 6):
        gather_v(k)
    pl.semaphore_wait(far_sem.at[0], 1)
    gather_q(7)
    pl.semaphore_wait(far_sem.at[1], 1)
    gather_v(7)
    def pass_on(ks):
        drain(vbuf.at[0 : len(ks)], q_recv.at[WAVE[ks[0]]])
        for k in ks:
            theirs = qbuf.at[a_chip[k][1], pl.ds(lo, ROWS)]
            send(theirs, theirs, big_send, f_recv.at[0 if k in NEAR else 1], other, dp)

    def weigh(part, first, last, ks):
        rows = slice(first * ROWS, last * ROWS)
        v_part = vbuf[first:last].reshape((last - first) * ROWS, D)
        for k in ks:
            c = a_chip[k][1]
            logits = lax.dot_general(v_part, qbuf[c], (((1,), (1,)), ((), ())), preferred_element_type=F32)
            e = jnp.exp(logits * INV_TEMP)
            spart[part, c, 0:1, :] = jnp.sum(e, axis=0, keepdims=True)
            t_ref[c, rows, :] = e.astype(BF16)

    pass_on(NEAR[1:])
    drain(vbuf.at[1:4], v_recv.at[0])
    drain(qbuf.at[0:2], f_recv.at[0])
    pass_on(FAR[:3])
    weigh(0, 0, 4, NEAR)
    pass_on(FAR[3:])
    drain(qbuf.at[0:2], f_recv.at[1])
    weigh(0, 0, 4, FAR)
    drain(vbuf.at[4:7], v_recv.at[1])
    weigh(1, 4, 7, range(8))
    drain(vbuf.at[7], v_recv.at[2])
    weigh(2, 7, 8, range(8))
    a_me = core * 8 + c_me
    for c in range(8):
        sbuf[a_me, c : c + 1, :] = spart[0, c, 0:1, :] + spart[1, c, 0:1, :] + spart[2, c, 0:1, :]
    v_all = vbuf[...].reshape(8 * ROWS, D)

    def exchange(ref, ssem, rsem):
        for k in ORDER:
            for blk in (core, other):
                send(ref, ref, ssem, rsem, blk, a_chip[k][0])
        send(ref, ref, ssem, rsem, other, dp)

    exchange(sbuf.at[a_me], s_send, s_recv)
    exchange(ybuf.at[a_me], small_send, y_recv)

    for c in range(8):
        ut = lax.dot_general(v_all, t_ref[c], (((0,), (0,)), ((), ())), preferred_element_type=F32)
        ub[0, c] = ut[:, :ROWS].astype(BF16)
        ub[1, c] = ut[:, ROWS:].astype(BF16)
    send(ub.at[other], ud, big_send, d_recv, other, dp)

    drain(ud, d_recv)
    for c in range(8):
        us[c] = (ub[core, c].astype(F32) + ud[c].astype(F32)).astype(BF16)
    for k in ORDER:
        send(us.at[a_chip[k][1]], ur.at[k], big_send, u_recv, core, a_chip[k][0])

    drain(sbuf.at[0:15], s_recv)
    total = sbuf[0]
    for a in range(1, 16):
        total = total + sbuf[a]
    inverse = 1.0 / total
    scales = [jnp.broadcast_to(inverse[c : c + 1, :], (1, 16, 2 * ROWS)).astype(BF16) for c in range(8)]

    def loss_rows():
        drain(ybuf.at[0:15], y_recv)
        hits = ybuf[0]
        for a in range(1, 16):
            hits = hits + ybuf[a]
        logs = jnp.sum(jnp.log(total), axis=0, keepdims=True)
        xbuf[b_me] = (logs[:, :ROWS] + logs[:, ROWS:]) - hits * INV_TEMP
        for k in ORDER:
            send(xbuf.at[b_me], xbuf.at[b_me], small_send, x_recv, core, b_chip[k])

    def pull(rows, n):
        acc = jnp.zeros((n, D), F32)
        for c in range(8):
            probs = rows(c).reshape(n // 16, 16, 2 * ROWS) * scales[c]
            acc = acc + jnp.dot(probs.reshape(n, 2 * ROWS), qbuf[c], preferred_element_type=F32)
        return acc

    def give(k, part, chip):
        wb[k] = part.astype(BF16)
        send(wb.at[k], wr.at[k], big_send, w_recv, core, chip)

    def keep(part):
        w_own[...] = part

    for n, targets in enumerate(W_ORDER):
        ks, rows, chips = [], [], []
        for b in targets:
            bits = ((b >> 2) & 1, (b >> 1) & 1, b & 1)
            dz, dy, dx = (1 - own if bit else own for bit, own in zip(bits, b_bits))
            k = 4 * dz + 2 * dy + dx
            slot = k - dz * (1 - dy) * (1 - dx) + (1 - dz) * dy * dx
            ks.append(k)
            rows.append(pl.ds(pl.multiple_of(slot * ROWS, ROWS), ROWS))
            chips.append(
                number(
                    [
                        (3 - low_bit(p) if bit else low_bit(p)) if is_low else high_bit(p) * (3 - 2 * bit) + bit
                        for p, bit, is_low in zip(place, bits, A_LOW)
                    ]
                )
            )
        acc = pull(lambda c: jnp.concatenate([t_ref[c, r, :] for r in rows]), len(targets) * ROWS)
        for m, b in enumerate(targets):
            part = acc[m * ROWS : (m + 1) * ROWS]
            pl.when(b_me == b)(functools.partial(keep, part))
            pl.when(b_me != b)(functools.partial(give, ks[m], part, chips[m]))
        if n == 0:
            loss_rows()

    mine = lax.broadcasted_iota(jnp.int32, total.shape, 0) == c_me
    s_row = jnp.sum(jnp.where(mine, total, 0.0), axis=0, keepdims=True)
    s_row = jnp.where(core == 0, s_row[:, :ROWS], s_row[:, ROWS:])

    def slope(pull, unit, length):
        along = jnp.sum(unit * pull, axis=1, keepdims=True)
        return (pull - unit * along) / length

    drain(ur.at[1:8], u_recv)
    u_sum = ub[core, c_me].astype(F32) + ud[c_me].astype(F32)
    for k in range(1, 8):
        u_sum = u_sum + ur[k].astype(F32)
    q_pull = (jnp.transpose(u_sum / s_row) - vbuf[0].astype(F32)) * INV_TEMP
    qs_ref[...] = slope(q_pull, q_unit[...], lens[0])

    drain(xbuf.at[0:7], x_recv)
    x_sum = xbuf[0]
    for b in range(1, 8):
        x_sum = x_sum + xbuf[b]
    hits_ref[...] = x_sum

    drain(t_ref.at[:, 0:704, :], big_send)
    drain(sbuf.at[0:15], s_send)
    drain(ybuf.at[0:22], small_send)

    drain(wr.at[1:8], w_recv)
    w_sum = w_own[...]
    for k in range(1, 8):
        w_sum = w_sum + wr[k].astype(F32)
    v_pull = (w_sum - qbuf[c_me, pl.ds(lo, ROWS), :].astype(F32)) * INV_TEMP
    cs_ref[...] = slope(v_pull, v_unit[...], lens[1])


def write_out(l_ref, q_ref, v_ref, l_out, q_out, v_out, l_own, sem):
    q_copy = pltpu.make_async_copy(q_ref, q_out, sem.at[0])
    v_copy = pltpu.make_async_copy(v_ref, v_out, sem.at[1])
    q_copy.start()
    v_copy.start()
    l_own[0, 0] = jnp.sum(l_ref[...]) / BATCH
    l_copy = pltpu.make_async_copy(l_own, l_out, sem.at[2])
    l_copy.start()
    l_copy.wait()
    q_copy.wait()
    v_copy.wait()


def per_device(queries, items):
    dma = pltpu.SemaphoreType.DMA
    vmem = pltpu.VMEM
    parts = pl.pallas_call(
        kernel,
        out_shape=(vmem((1, ROWS), F32), vmem((ROWS, D), F32), vmem((ROWS, D), F32)),
        in_specs=[pl.BlockSpec(memory_space=pltpu.HBM)] * 2,
        out_specs=(pl.BlockSpec(memory_space=vmem),) * 3,
        scratch_shapes=[
            vmem((2, ROWS, D), BF16),
            vmem((ROWS, D), F32),
            vmem((ROWS, D), F32),
            vmem((2, ROWS, 1), F32),
            vmem((8, 2 * ROWS, D), BF16),
            vmem((8, ROWS, D), BF16),
            vmem((8, 8 * ROWS, 2 * ROWS), BF16),
            vmem((16, 8, 2 * ROWS), F32),
            vmem((3, 8, 8, 2 * ROWS), F32),
            vmem((2, 8, D, ROWS), BF16),
            vmem((8, D, ROWS), BF16),
            vmem((8, D, ROWS), BF16),
            vmem((8, D, ROWS), BF16),
            vmem((8, ROWS, D), BF16),
            vmem((ROWS, D), F32),
            vmem((8, ROWS, D), BF16),
            vmem((8, 1, ROWS), F32),
            vmem((24, 1, ROWS), F32),
            dma,
            dma((3,)),
            dma((2,)),
            dma((3,)),
            dma,
            dma,
            dma,
            dma,
            dma,
            dma,
            dma,
            dma,
            dma,
            pltpu.SemaphoreType.REGULAR((2,)),
            pltpu.SemaphoreType.REGULAR((2,)),
        ],
        compiler_params=pltpu.CompilerParams(collective_id=0, has_side_effects=True),
    )(queries, items)
    loss, q_slope, v_slope = pl.pallas_call(
        write_out,
        out_shape=(
            jax.ShapeDtypeStruct((1, 1), F32),
            jax.ShapeDtypeStruct((ROWS, D), F32),
            jax.ShapeDtypeStruct((ROWS, D), F32),
        ),
        in_specs=[pl.BlockSpec(memory_space=vmem)] * 3,
        out_specs=(
            pl.BlockSpec(memory_space=pltpu.HBM),
            pl.BlockSpec(memory_space=pltpu.HBM),
            pl.BlockSpec(memory_space=pltpu.HBM),
        ),
        scratch_shapes=[pltpu.SMEM((1, 1), F32), dma((3,))],
        compiler_params=pltpu.CompilerParams(vmem_limit_bytes=1024 * 1024),
    )(*(pltpu.with_memory_space_constraint(part, vmem) for part in parts))
    return loss.reshape(()), q_slope, v_slope


def solution(mesh):
    spec = P(("blk", "dp"), None)
    return jax.shard_map(
        per_device, mesh=mesh, in_specs=(spec, spec), out_specs=(P(), spec, spec), check_vma=False
    )
```

```python
import functools

import jax
import jax.numpy as jnp
from jax import lax
from jax.experimental import pallas as pl
from jax.experimental.pallas import tpu as pltpu
from jax.sharding import PartitionSpec as P

MESH = pl.DeviceIdType.MESH
ROWS = 128
D = 256
BATCH = 16384
INV_TEMP = 20.0
LOG2_E = 1.4426950408889634
TINY = 1e-12
F32 = jnp.float32
BF16 = jnp.bfloat16
A_LOW = (True, False, True)
SLOT = (0, 1, 2, 4, 3, 5, 6, 7)
NEAR, FAR = (0, 1, 2, 4), (3, 5, 6, 7)
WAVE = (None, 0, 0, 1, 0, 1, 1, 2)
W_ORDER = ((0,), (2, 1), (4, 3), (6, 7), (5,))
ORDER = (7, 3, 5, 6, 1, 2, 4)


def flip_low(p, d):
    return p + 1 - 2 * (p & 1) if d else p


def flip_high(p, d):
    return 3 - p if d else p


def low_bit(p):
    return ((p + 1) >> 1) & 1


def high_bit(p):
    return p >> 1


def kernel(
    q_hbm,
    v_hbm,
    hits_ref,
    qs_ref,
    cs_ref,
    given,
    q_unit,
    v_unit,
    lens,
    qbuf,
    vbuf,
    t_ref,
    sbuf,
    spart,
    ub,
    ud,
    us,
    ur,
    wb,
    w_own,
    wr,
    xbuf,
    ybuf,
    in_sem,
    q_recv,
    f_recv,
    v_recv,
    big_send,
    small_send,
    s_send,
    s_recv,
    d_recv,
    u_recv,
    w_recv,
    x_recv,
    y_recv,
    near_sem,
    far_sem,
):
    core = lax.axis_index("blk")
    other = 1 - core
    dp = lax.axis_index("dp")
    z, y, x = dp >> 4, (dp >> 2) & 3, dp & 3

    place = (z, y, x)

    def partner(k, low):
        steps = ((k >> 2) & 1, (k >> 1) & 1, k & 1)
        zz, yy, xx = (
            (flip_low if is_low == low else flip_high)(p, d) for p, d, is_low in zip(place, steps, A_LOW)
        )
        return zz, yy, xx

    def rank(place, low):
        bits = [(low_bit if is_low == low else high_bit)(p) for p, is_low in zip(place, A_LOW)]
        return bits[0] * 4 + bits[1] * 2 + bits[2]

    def number(place):
        return place[0] * 16 + place[1] * 4 + place[2]

    a_place = {k: partner(k, True) for k in (1, 2, 4)}
    b_place = {k: partner(k, False) for k in (1, 2, 4)}
    barrier = pltpu.get_barrier_semaphore()

    def tell(sem, blk, chip):
        pl.semaphore_signal(sem, inc=1, device_id=(blk, chip), device_id_type=MESH)

    tell(barrier, other, dp)
    for k in (1, 2, 4):
        tell(barrier, core, number(b_place[k]))
        tell(barrier, core, number(a_place[k]))

    pltpu.make_async_copy(q_hbm, given.at[0], in_sem).start()
    pltpu.make_async_copy(v_hbm, given.at[1], in_sem).start()

    a_chip = [(number(partner(k, True)), rank(partner(k, True), True)) for k in range(8)]
    b_chip = [number(partner(k, False)) for k in range(8)]
    c_me = a_chip[0][1]
    b_me = rank(place, False)

    b_bits = [high_bit(p) if is_low else low_bit(p) for p, is_low in zip(place, A_LOW)]
    lo = pl.multiple_of(core * ROWS, ROWS)

    def plan(src, dst, ssem, rsem, blk, chip):
        return pltpu.make_async_remote_copy(
            src_ref=src, dst_ref=dst, send_sem=ssem, recv_sem=rsem, device_id=(blk, chip), device_id_type=MESH
        )

    def send(*where):
        plan(*where).start()

    def drain(ref, sem):
        pltpu.make_async_copy(ref, ref, sem).wait()

    drain(given, in_sem)

    def unit_rows(value):
        wide = value.astype(F32)
        length = jnp.sqrt(jnp.sum(wide * wide, axis=1, keepdims=True) + TINY)
        return wide / length, length

    qu, ql = unit_rows(given[0])
    vu, vl = unit_rows(given[1])
    q_hat, v_hat = qu.astype(BF16), vu.astype(BF16)
    q_unit[...] = qu
    v_unit[...] = vu
    lens[0] = ql
    lens[1] = vl
    q_own = qbuf.at[c_me, pl.ds(lo, ROWS)]
    qbuf[c_me, pl.ds(lo, ROWS), :] = q_hat
    vbuf[0] = v_hat
    hits = jnp.sum(q_hat.astype(F32) * v_hat.astype(F32), axis=0, keepdims=True)
    ybuf[core * 8 + c_me] = hits[:, :ROWS] + hits[:, ROWS:]

    pl.semaphore_wait(barrier, 7)
    for d in range(3):
        tell(near_sem.at[0], core, a_chip[1 << d][0])
        tell(near_sem.at[1], core, b_chip[1 << d])

    def gather_q(k):
        send(q_own, q_own, big_send, q_recv.at[WAVE[k]], core, a_chip[k][0])

    def gather_v(k):
        send(vbuf.at[0], vbuf.at[SLOT[k]], big_send, v_recv.at[WAVE[k]], core, b_chip[k])

    send(q_own, q_own, big_send, f_recv.at[0], other, dp)
    for k in (1, 2, 4):
        gather_v(k)
        gather_q(k)
    pl.semaphore_wait(near_sem.at[0], 3)
    tell(far_sem.at[0], core, a_chip[1][0])
    for k in (3, 5, 6):
        gather_q(k)
    pl.semaphore_wait(near_sem.at[1], 3)
    tell(far_sem.at[1], core, b_chip[1])
    for k in (3, 5, 6):
        gather_v(k)
    pl.semaphore_wait(far_sem.at[0], 1)
    gather_q(7)
    pl.semaphore_wait(far_sem.at[1], 1)
    gather_v(7)
    def pass_on(ks):
        drain(vbuf.at[0 : len(ks)], q_recv.at[WAVE[ks[0]]])
        for k in ks:
            theirs = qbuf.at[a_chip[k][1], pl.ds(lo, ROWS)]
            send(theirs, theirs, big_send, f_recv.at[0 if k in NEAR else 1], other, dp)

    def weigh(part, first, last, ks):
        rows = slice(first * ROWS, last * ROWS)
        v_part = vbuf[first:last].reshape((last - first) * ROWS, D)
        for k in ks:
            c = a_chip[k][1]
            logits = lax.dot_general(v_part, qbuf[c], (((1,), (1,)), ((), ())), preferred_element_type=F32)
            e = jnp.exp2(logits * (INV_TEMP * LOG2_E))
            spart[part, c, 0:1, :] = jnp.sum(e, axis=0, keepdims=True)
            t_ref[c, rows, :] = e.astype(BF16)

    pass_on(NEAR[1:])
    drain(vbuf.at[1:4], v_recv.at[0])
    drain(qbuf.at[0:2], f_recv.at[0])
    pass_on(FAR[:3])
    weigh(0, 0, 4, NEAR)
    pass_on(FAR[3:])
    drain(qbuf.at[0:2], f_recv.at[1])
    weigh(0, 0, 4, FAR)
    drain(vbuf.at[4:7], v_recv.at[1])
    weigh(1, 4, 7, range(8))
    drain(vbuf.at[7], v_recv.at[2])
    weigh(2, 7, 8, range(8))
    a_me = core * 8 + c_me
    for c in range(8):
        sbuf[a_me, c : c + 1, :] = spart[0, c, 0:1, :] + spart[1, c, 0:1, :] + spart[2, c, 0:1, :]
    v_all = vbuf[...].reshape(8 * ROWS, D)

    def exchange(ref, ssem, rsem):
        for k in ORDER:
            for blk in (core, other):
                send(ref, ref, ssem, rsem, blk, a_chip[k][0])
        send(ref, ref, ssem, rsem, other, dp)

    exchange(sbuf.at[a_me], s_send, s_recv)
    exchange(ybuf.at[a_me], small_send, y_recv)

    for c in range(8):
        ut = lax.dot_general(v_all, t_ref[c], (((0,), (0,)), ((), ())), preferred_element_type=F32)
        ub[0, c] = ut[:, :ROWS].astype(BF16)
        ub[1, c] = ut[:, ROWS:].astype(BF16)
    send(ub.at[other], ud, big_send, d_recv, other, dp)

    drain(ud, d_recv)
    for c in range(8):
        us[c] = (ub[core, c].astype(F32) + ud[c].astype(F32)).astype(BF16)
    for k in ORDER:
        send(us.at[a_chip[k][1]], ur.at[k], big_send, u_recv, core, a_chip[k][0])

    drain(sbuf.at[0:15], s_recv)
    total = sbuf[0]
    for a in range(1, 16):
        total = total + sbuf[a]
    inverse = 1.0 / total
    scales = [jnp.broadcast_to(inverse[c : c + 1, :], (1, 16, 2 * ROWS)).astype(BF16) for c in range(8)]

    def loss_rows():
        drain(ybuf.at[0:15], y_recv)
        hits = ybuf[0]
        for a in range(1, 16):
            hits = hits + ybuf[a]
        logs = jnp.sum(jnp.log(total), axis=0, keepdims=True)
        xbuf[b_me] = (logs[:, :ROWS] + logs[:, ROWS:]) - hits * INV_TEMP
        for k in ORDER:
            send(xbuf.at[b_me], xbuf.at[b_me], small_send, x_recv, core, b_chip[k])

    def pull(rows, n):
        acc = jnp.zeros((n, D), F32)
        for c in range(8):
            probs = rows(c).reshape(n // 16, 16, 2 * ROWS) * scales[c]
            acc = acc + jnp.dot(probs.reshape(n, 2 * ROWS), qbuf[c], preferred_element_type=F32)
        return acc

    def give(k, part, chip):
        wb[k] = part.astype(BF16)
        send(wb.at[k], wr.at[k], big_send, w_recv, core, chip)

    def keep(part):
        w_own[...] = part

    for n, targets in enumerate(W_ORDER):
        ks, rows, chips = [], [], []
        for b in targets:
            bits = ((b >> 2) & 1, (b >> 1) & 1, b & 1)
            dz, dy, dx = (1 - own if bit else own for bit, own in zip(bits, b_bits))
            k = 4 * dz + 2 * dy + dx
            slot = k - dz * (1 - dy) * (1 - dx) + (1 - dz) * dy * dx
            ks.append(k)
            rows.append(pl.ds(pl.multiple_of(slot * ROWS, ROWS), ROWS))
            chips.append(
                number(
                    [
                        (3 - low_bit(p) if bit else low_bit(p)) if is_low else high_bit(p) * (3 - 2 * bit) + bit
                        for p, bit, is_low in zip(place, bits, A_LOW)
                    ]
                )
            )
        acc = pull(lambda c: jnp.concatenate([t_ref[c, r, :] for r in rows]), len(targets) * ROWS)
        for m, b in enumerate(targets):
            part = acc[m * ROWS : (m + 1) * ROWS]
            pl.when(b_me == b)(functools.partial(keep, part))
            pl.when(b_me != b)(functools.partial(give, ks[m], part, chips[m]))
        if n == 0:
            loss_rows()

    mine = lax.broadcasted_iota(jnp.int32, total.shape, 0) == c_me
    s_row = jnp.sum(jnp.where(mine, total, 0.0), axis=0, keepdims=True)
    s_row = jnp.where(core == 0, s_row[:, :ROWS], s_row[:, ROWS:])

    def slope(pull, unit, length):
        along = jnp.sum(unit * pull, axis=1, keepdims=True)
        return (pull - unit * along) / length

    drain(ur.at[1:8], u_recv)
    u_sum = ub[core, c_me].astype(F32) + ud[c_me].astype(F32)
    for k in range(1, 8):
        u_sum = u_sum + ur[k].astype(F32)
    q_pull = (jnp.transpose(u_sum / s_row) - vbuf[0].astype(F32)) * INV_TEMP
    qs_ref[...] = slope(q_pull, q_unit[...], lens[0])

    drain(xbuf.at[0:7], x_recv)
    x_sum = xbuf[0]
    for b in range(1, 8):
        x_sum = x_sum + xbuf[b]
    hits_ref[...] = x_sum

    drain(t_ref.at[:, 0:704, :], big_send)
    drain(sbuf.at[0:15], s_send)
    drain(ybuf.at[0:22], small_send)

    drain(wr.at[1:8], w_recv)
    w_sum = w_own[...]
    for k in range(1, 8):
        w_sum = w_sum + wr[k].astype(F32)
    v_pull = (w_sum - qbuf[c_me, pl.ds(lo, ROWS), :].astype(F32)) * INV_TEMP
    cs_ref[...] = slope(v_pull, v_unit[...], lens[1])


def write_out(l_ref, q_ref, v_ref, l_out, q_out, v_out, l_own, sem):
    q_copy = pltpu.make_async_copy(q_ref, q_out, sem.at[0])
    v_copy = pltpu.make_async_copy(v_ref, v_out, sem.at[1])
    q_copy.start()
    v_copy.start()
    l_own[0, 0] = jnp.sum(l_ref[...]) / BATCH
    l_copy = pltpu.make_async_copy(l_own, l_out, sem.at[2])
    l_copy.start()
    l_copy.wait()
    q_copy.wait()
    v_copy.wait()


def per_device(queries, items):
    dma = pltpu.SemaphoreType.DMA
    vmem = pltpu.VMEM
    parts = pl.pallas_call(
        kernel,
        out_shape=(vmem((1, ROWS), F32), vmem((ROWS, D), F32), vmem((ROWS, D), F32)),
        in_specs=[pl.BlockSpec(memory_space=pltpu.HBM)] * 2,
        out_specs=(pl.BlockSpec(memory_space=vmem),) * 3,
        scratch_shapes=[
            vmem((2, ROWS, D), BF16),
            vmem((ROWS, D), F32),
            vmem((ROWS, D), F32),
            vmem((2, ROWS, 1), F32),
            vmem((8, 2 * ROWS, D), BF16),
            vmem((8, ROWS, D), BF16),
            vmem((8, 8 * ROWS, 2 * ROWS), BF16),
            vmem((16, 8, 2 * ROWS), F32),
            vmem((3, 8, 8, 2 * ROWS), F32),
            vmem((2, 8, D, ROWS), BF16),
            vmem((8, D, ROWS), BF16),
            vmem((8, D, ROWS), BF16),
            vmem((8, D, ROWS), BF16),
            vmem((8, ROWS, D), BF16),
            vmem((ROWS, D), F32),
            vmem((8, ROWS, D), BF16),
            vmem((8, 1, ROWS), F32),
            vmem((24, 1, ROWS), F32),
            dma,
            dma((3,)),
            dma((2,)),
            dma((3,)),
            dma,
            dma,
            dma,
            dma,
            dma,
            dma,
            dma,
            dma,
            dma,
            pltpu.SemaphoreType.REGULAR((2,)),
            pltpu.SemaphoreType.REGULAR((2,)),
        ],
        compiler_params=pltpu.CompilerParams(collective_id=0, has_side_effects=True),
    )(queries, items)
    loss, q_slope, v_slope = pl.pallas_call(
        write_out,
        out_shape=(
            jax.ShapeDtypeStruct((1, 1), F32),
            jax.ShapeDtypeStruct((ROWS, D), F32),
            jax.ShapeDtypeStruct((ROWS, D), F32),
        ),
        in_specs=[pl.BlockSpec(memory_space=vmem)] * 3,
        out_specs=(
            pl.BlockSpec(memory_space=pltpu.HBM),
            pl.BlockSpec(memory_space=pltpu.HBM),
            pl.BlockSpec(memory_space=pltpu.HBM),
        ),
        scratch_shapes=[pltpu.SMEM((1, 1), F32), dma((3,))],
        compiler_params=pltpu.CompilerParams(vmem_limit_bytes=1024 * 1024),
    )(*(pltpu.with_memory_space_constraint(part, vmem) for part in parts))
    return loss.reshape(()), q_slope, v_slope


def solution(mesh):
    spec = P(("blk", "dp"), None)
    return jax.shard_map(
        per_device, mesh=mesh, in_specs=(spec, spec), out_specs=(P(), spec, spec), check_vma=False
    )
```

```python
import functools

import jax
import jax.numpy as jnp
from jax import lax
from jax.experimental import pallas as pl
from jax.experimental.pallas import tpu as pltpu
from jax.sharding import PartitionSpec as P

MESH = pl.DeviceIdType.MESH
ROWS = 128
D = 256
BATCH = 16384
INV_TEMP = 20.0
LOG2_E = 1.4426950408889634
TINY = 1e-12
F32 = jnp.float32
BF16 = jnp.bfloat16
A_LOW = (True, False, True)
SLOT = (0, 1, 2, 4, 3, 5, 6, 7)
NEAR, FAR = (0, 1, 2, 4), (3, 5, 6, 7)
WAVE = (None, 0, 0, 1, 0, 1, 1, 2)
W_ORDER = ((0,), (2, 1), (4, 3), (6, 7), (5,))
ORDER = (7, 3, 5, 6, 1, 2, 4)


def flip_low(p, d):
    return p + 1 - 2 * (p & 1) if d else p


def flip_high(p, d):
    return 3 - p if d else p


def low_bit(p):
    return ((p + 1) >> 1) & 1


def high_bit(p):
    return p >> 1


def kernel(
    q_hbm,
    v_hbm,
    hits_ref,
    qs_ref,
    cs_ref,
    given,
    q_unit,
    v_unit,
    lens,
    qbuf,
    vbuf,
    t_ref,
    sbuf,
    spart,
    ub,
    ud,
    us,
    ur,
    wb,
    w_own,
    wr,
    xbuf,
    ybuf,
    in_sem,
    q_recv,
    f_recv,
    v_recv,
    big_send,
    small_send,
    s_send,
    s_recv,
    d_recv,
    u_recv,
    w_recv,
    x_recv,
    y_recv,
    near_sem,
    far_sem,
):
    core = lax.axis_index("blk")
    other = 1 - core
    dp = lax.axis_index("dp")
    z, y, x = dp >> 4, (dp >> 2) & 3, dp & 3

    place = (z, y, x)

    def partner(k, low):
        steps = ((k >> 2) & 1, (k >> 1) & 1, k & 1)
        zz, yy, xx = (
            (flip_low if is_low == low else flip_high)(p, d) for p, d, is_low in zip(place, steps, A_LOW)
        )
        return zz, yy, xx

    def rank(place, low):
        bits = [(low_bit if is_low == low else high_bit)(p) for p, is_low in zip(place, A_LOW)]
        return bits[0] * 4 + bits[1] * 2 + bits[2]

    def number(place):
        return place[0] * 16 + place[1] * 4 + place[2]

    a_place = {k: partner(k, True) for k in (1, 2, 4)}
    b_place = {k: partner(k, False) for k in (1, 2, 4)}
    barrier = pltpu.get_barrier_semaphore()

    def tell(sem, blk, chip):
        pl.semaphore_signal(sem, inc=1, device_id=(blk, chip), device_id_type=MESH)

    tell(barrier, other, dp)
    for k in (1, 2, 4):
        tell(barrier, core, number(b_place[k]))
        tell(barrier, core, number(a_place[k]))

    pltpu.make_async_copy(q_hbm, given.at[0], in_sem).start()
    pltpu.make_async_copy(v_hbm, given.at[1], in_sem).start()

    a_chip = [(number(partner(k, True)), rank(partner(k, True), True)) for k in range(8)]
    b_chip = [number(partner(k, False)) for k in range(8)]
    c_me = a_chip[0][1]
    b_me = rank(place, False)

    b_bits = [high_bit(p) if is_low else low_bit(p) for p, is_low in zip(place, A_LOW)]
    lo = pl.multiple_of(core * ROWS, ROWS)

    def plan(src, dst, ssem, rsem, blk, chip):
        return pltpu.make_async_remote_copy(
            src_ref=src, dst_ref=dst, send_sem=ssem, recv_sem=rsem, device_id=(blk, chip), device_id_type=MESH
        )

    def send(*where):
        plan(*where).start()

    def drain(ref, sem):
        pltpu.make_async_copy(ref, ref, sem).wait()

    drain(given, in_sem)

    def unit_rows(value):
        wide = value.astype(F32)
        length = jnp.sqrt(jnp.sum(wide * wide, axis=1, keepdims=True) + TINY)
        return wide / length, length

    qu, ql = unit_rows(given[0])
    vu, vl = unit_rows(given[1])
    q_hat, v_hat = qu.astype(BF16), vu.astype(BF16)
    q_unit[...] = qu
    v_unit[...] = vu
    lens[0] = ql
    lens[1] = vl
    q_own = qbuf.at[c_me, pl.ds(lo, ROWS)]
    qbuf[c_me, pl.ds(lo, ROWS), :] = q_hat
    vbuf[0] = v_hat
    hits = jnp.sum(q_hat.astype(F32) * v_hat.astype(F32), axis=0, keepdims=True)
    ybuf[core * 8 + c_me] = hits[:, :ROWS] + hits[:, ROWS:]

    pl.semaphore_wait(barrier, 7)
    for d in range(3):
        tell(near_sem.at[0], core, a_chip[1 << d][0])
        tell(near_sem.at[1], core, b_chip[1 << d])

    def gather_q(k):
        send(q_own, q_own, big_send, q_recv.at[WAVE[k]], core, a_chip[k][0])

    def gather_v(k):
        send(vbuf.at[0], vbuf.at[SLOT[k]], big_send, v_recv.at[WAVE[k]], core, b_chip[k])

    send(q_own, q_own, big_send, f_recv.at[0], other, dp)
    for k in (4, 2, 1):
        gather_v(k)
        gather_q(k)
    pl.semaphore_wait(near_sem.at[0], 3)
    tell(far_sem.at[0], core, a_chip[1][0])
    for k in (6, 5, 3):
        gather_q(k)
    pl.semaphore_wait(near_sem.at[1], 3)
    tell(far_sem.at[1], core, b_chip[1])
    for k in (6, 5, 3):
        gather_v(k)
    pl.semaphore_wait(far_sem.at[0], 1)
    gather_q(7)
    pl.semaphore_wait(far_sem.at[1], 1)
    gather_v(7)
    def pass_on(ks):
        drain(vbuf.at[0 : len(ks)], q_recv.at[WAVE[ks[0]]])
        for k in ks:
            theirs = qbuf.at[a_chip[k][1], pl.ds(lo, ROWS)]
            send(theirs, theirs, big_send, f_recv.at[0 if k in NEAR else 1], other, dp)

    def weigh(part, first, last, ks):
        rows = slice(first * ROWS, last * ROWS)
        v_part = vbuf[first:last].reshape((last - first) * ROWS, D)
        for k in ks:
            c = a_chip[k][1]
            logits = lax.dot_general(v_part, qbuf[c], (((1,), (1,)), ((), ())), preferred_element_type=F32)
            e = jnp.exp2(logits * (INV_TEMP * LOG2_E))
            spart[part, c, 0:1, :] = jnp.sum(e, axis=0, keepdims=True)
            t_ref[c, rows, :] = e.astype(BF16)

    pass_on(NEAR[1:])
    drain(vbuf.at[1:4], v_recv.at[0])
    drain(qbuf.at[0:2], f_recv.at[0])
    pass_on(FAR[:3])
    weigh(0, 0, 4, NEAR)
    pass_on(FAR[3:])
    drain(qbuf.at[0:2], f_recv.at[1])
    weigh(0, 0, 4, FAR)
    drain(vbuf.at[4:7], v_recv.at[1])
    weigh(1, 4, 7, range(8))
    drain(vbuf.at[7], v_recv.at[2])
    weigh(2, 7, 8, range(8))
    a_me = core * 8 + c_me
    for c in range(8):
        sbuf[a_me, c : c + 1, :] = spart[0, c, 0:1, :] + spart[1, c, 0:1, :] + spart[2, c, 0:1, :]
    v_all = vbuf[...].reshape(8 * ROWS, D)

    def exchange(ref, ssem, rsem):
        for k in ORDER:
            for blk in (core, other):
                send(ref, ref, ssem, rsem, blk, a_chip[k][0])
        send(ref, ref, ssem, rsem, other, dp)

    exchange(sbuf.at[a_me], s_send, s_recv)
    exchange(ybuf.at[a_me], small_send, y_recv)

    for c in range(8):
        ut = lax.dot_general(v_all, t_ref[c], (((0,), (0,)), ((), ())), preferred_element_type=F32)
        ub[0, c] = ut[:, :ROWS].astype(BF16)
        ub[1, c] = ut[:, ROWS:].astype(BF16)
    send(ub.at[other], ud, big_send, d_recv, other, dp)

    drain(ud, d_recv)
    for c in range(8):
        us[c] = (ub[core, c].astype(F32) + ud[c].astype(F32)).astype(BF16)
    for k in ORDER:
        send(us.at[a_chip[k][1]], ur.at[k], big_send, u_recv, core, a_chip[k][0])

    drain(sbuf.at[0:15], s_recv)
    total = sbuf[0]
    for a in range(1, 16):
        total = total + sbuf[a]
    inverse = 1.0 / total
    scales = [jnp.broadcast_to(inverse[c : c + 1, :], (1, 16, 2 * ROWS)).astype(BF16) for c in range(8)]

    def loss_rows():
        drain(ybuf.at[0:15], y_recv)
        hits = ybuf[0]
        for a in range(1, 16):
            hits = hits + ybuf[a]
        logs = jnp.sum(jnp.log(total), axis=0, keepdims=True)
        xbuf[b_me] = (logs[:, :ROWS] + logs[:, ROWS:]) - hits * INV_TEMP
        for k in ORDER:
            send(xbuf.at[b_me], xbuf.at[b_me], small_send, x_recv, core, b_chip[k])

    def pull(rows, n):
        acc = jnp.zeros((n, D), F32)
        for c in range(8):
            probs = rows(c).reshape(n // 16, 16, 2 * ROWS) * scales[c]
            acc = acc + jnp.dot(probs.reshape(n, 2 * ROWS), qbuf[c], preferred_element_type=F32)
        return acc

    def give(k, part, chip):
        wb[k] = part.astype(BF16)
        send(wb.at[k], wr.at[k], big_send, w_recv, core, chip)

    def keep(part):
        w_own[...] = part

    for n, targets in enumerate(W_ORDER):
        ks, rows, chips = [], [], []
        for b in targets:
            bits = ((b >> 2) & 1, (b >> 1) & 1, b & 1)
            dz, dy, dx = (1 - own if bit else own for bit, own in zip(bits, b_bits))
            k = 4 * dz + 2 * dy + dx
            slot = k - dz * (1 - dy) * (1 - dx) + (1 - dz) * dy * dx
            ks.append(k)
            rows.append(pl.ds(pl.multiple_of(slot * ROWS, ROWS), ROWS))
            chips.append(
                number(
                    [
                        (3 - low_bit(p) if bit else low_bit(p)) if is_low else high_bit(p) * (3 - 2 * bit) + bit
                        for p, bit, is_low in zip(place, bits, A_LOW)
                    ]
                )
            )
        acc = pull(lambda c: jnp.concatenate([t_ref[c, r, :] for r in rows]), len(targets) * ROWS)
        for m, b in enumerate(targets):
            part = acc[m * ROWS : (m + 1) * ROWS]
            pl.when(b_me == b)(functools.partial(keep, part))
            pl.when(b_me != b)(functools.partial(give, ks[m], part, chips[m]))
        if n == 0:
            loss_rows()

    mine = lax.broadcasted_iota(jnp.int32, total.shape, 0) == c_me
    s_row = jnp.sum(jnp.where(mine, total, 0.0), axis=0, keepdims=True)
    s_row = jnp.where(core == 0, s_row[:, :ROWS], s_row[:, ROWS:])

    def slope(pull, unit, length):
        along = jnp.sum(unit * pull, axis=1, keepdims=True)
        return (pull - unit * along) / length

    drain(ur.at[1:8], u_recv)
    u_sum = ub[core, c_me].astype(F32) + ud[c_me].astype(F32)
    for k in range(1, 8):
        u_sum = u_sum + ur[k].astype(F32)
    q_pull = (jnp.transpose(u_sum / s_row) - vbuf[0].astype(F32)) * INV_TEMP
    qs_ref[...] = slope(q_pull, q_unit[...], lens[0])

    drain(xbuf.at[0:7], x_recv)
    x_sum = xbuf[0]
    for b in range(1, 8):
        x_sum = x_sum + xbuf[b]
    hits_ref[...] = x_sum

    drain(t_ref.at[:, 0:704, :], big_send)
    drain(sbuf.at[0:15], s_send)
    drain(ybuf.at[0:22], small_send)

    drain(wr.at[1:8], w_recv)
    w_sum = w_own[...]
    for k in range(1, 8):
        w_sum = w_sum + wr[k].astype(F32)
    v_pull = (w_sum - qbuf[c_me, pl.ds(lo, ROWS), :].astype(F32)) * INV_TEMP
    cs_ref[...] = slope(v_pull, v_unit[...], lens[1])


def write_out(l_ref, q_ref, v_ref, l_out, q_out, v_out, l_own, sem):
    q_copy = pltpu.make_async_copy(q_ref, q_out, sem.at[0])
    v_copy = pltpu.make_async_copy(v_ref, v_out, sem.at[1])
    q_copy.start()
    v_copy.start()
    l_own[0, 0] = jnp.sum(l_ref[...]) / BATCH
    l_copy = pltpu.make_async_copy(l_own, l_out, sem.at[2])
    l_copy.start()
    l_copy.wait()
    q_copy.wait()
    v_copy.wait()


def per_device(queries, items):
    dma = pltpu.SemaphoreType.DMA
    vmem = pltpu.VMEM
    parts = pl.pallas_call(
        kernel,
        out_shape=(vmem((1, ROWS), F32), vmem((ROWS, D), F32), vmem((ROWS, D), F32)),
        in_specs=[pl.BlockSpec(memory_space=pltpu.HBM)] * 2,
        out_specs=(pl.BlockSpec(memory_space=vmem),) * 3,
        scratch_shapes=[
            vmem((2, ROWS, D), BF16),
            vmem((ROWS, D), F32),
            vmem((ROWS, D), F32),
            vmem((2, ROWS, 1), F32),
            vmem((8, 2 * ROWS, D), BF16),
            vmem((8, ROWS, D), BF16),
            vmem((8, 8 * ROWS, 2 * ROWS), BF16),
            vmem((16, 8, 2 * ROWS), F32),
            vmem((3, 8, 8, 2 * ROWS), F32),
            vmem((2, 8, D, ROWS), BF16),
            vmem((8, D, ROWS), BF16),
            vmem((8, D, ROWS), BF16),
            vmem((8, D, ROWS), BF16),
            vmem((8, ROWS, D), BF16),
            vmem((ROWS, D), F32),
            vmem((8, ROWS, D), BF16),
            vmem((8, 1, ROWS), F32),
            vmem((24, 1, ROWS), F32),
            dma,
            dma((3,)),
            dma((2,)),
            dma((3,)),
            dma,
            dma,
            dma,
            dma,
            dma,
            dma,
            dma,
            dma,
            dma,
            pltpu.SemaphoreType.REGULAR((2,)),
            pltpu.SemaphoreType.REGULAR((2,)),
        ],
        compiler_params=pltpu.CompilerParams(collective_id=0, has_side_effects=True),
    )(queries, items)
    loss, q_slope, v_slope = pl.pallas_call(
        write_out,
        out_shape=(
            jax.ShapeDtypeStruct((1, 1), F32),
            jax.ShapeDtypeStruct((ROWS, D), F32),
            jax.ShapeDtypeStruct((ROWS, D), F32),
        ),
        in_specs=[pl.BlockSpec(memory_space=vmem)] * 3,
        out_specs=(
            pl.BlockSpec(memory_space=pltpu.HBM),
            pl.BlockSpec(memory_space=pltpu.HBM),
            pl.BlockSpec(memory_space=pltpu.HBM),
        ),
        scratch_shapes=[pltpu.SMEM((1, 1), F32), dma((3,))],
        compiler_params=pltpu.CompilerParams(vmem_limit_bytes=1024 * 1024),
    )(*(pltpu.with_memory_space_constraint(part, vmem) for part in parts))
    return loss.reshape(()), q_slope, v_slope


def solution(mesh):
    spec = P(("blk", "dp"), None)
    return jax.shard_map(
        per_device, mesh=mesh, in_specs=(spec, spec), out_specs=(P(), spec, spec), check_vma=False
    )
```

```python
import functools

import jax
import jax.numpy as jnp
from jax import lax
from jax.experimental import pallas as pl
from jax.experimental.pallas import tpu as pltpu
from jax.sharding import PartitionSpec as P

MESH = pl.DeviceIdType.MESH
ROWS = 128
D = 256
BATCH = 16384
INV_TEMP = 20.0
LOG2_E = 1.4426950408889634
TINY = 1e-12
F32 = jnp.float32
BF16 = jnp.bfloat16
A_LOW = (True, True, True)
SLOT = (0, 1, 2, 4, 3, 5, 6, 7)
NEAR, FAR = (0, 1, 2, 4), (3, 5, 6, 7)
WAVE = (None, 0, 0, 1, 0, 1, 1, 2)
W_ORDER = ((0,), (1, 2), (4, 3), (5, 6), (7,))
ORDER = (7, 3, 5, 6, 1, 2, 4)


def flip_low(p, d):
    return p + 1 - 2 * (p & 1) if d else p


def flip_high(p, d):
    return 3 - p if d else p


def low_bit(p):
    return ((p + 1) >> 1) & 1


def high_bit(p):
    return p >> 1


def kernel(
    q_hbm,
    v_hbm,
    hits_ref,
    qs_ref,
    cs_ref,
    given,
    q_unit,
    v_unit,
    lens,
    qbuf,
    vbuf,
    t_ref,
    sbuf,
    spart,
    ub,
    ud,
    us,
    ur,
    wb,
    w_own,
    wr,
    xbuf,
    ybuf,
    in_sem,
    q_recv,
    f_recv,
    v_recv,
    big_send,
    small_send,
    s_send,
    s_recv,
    d_recv,
    u_recv,
    w_recv,
    x_recv,
    y_recv,
    near_sem,
    far_sem,
):
    core = lax.axis_index("blk")
    other = 1 - core
    dp = lax.axis_index("dp")
    z, y, x = dp >> 4, (dp >> 2) & 3, dp & 3

    place = (z, y, x)

    def partner(k, low):
        steps = ((k >> 2) & 1, (k >> 1) & 1, k & 1)
        zz, yy, xx = (
            (flip_low if is_low == low else flip_high)(p, d) for p, d, is_low in zip(place, steps, A_LOW)
        )
        return zz, yy, xx

    def rank(place, low):
        bits = [(low_bit if is_low == low else high_bit)(p) for p, is_low in zip(place, A_LOW)]
        return bits[0] * 4 + bits[1] * 2 + bits[2]

    def number(place):
        return place[0] * 16 + place[1] * 4 + place[2]

    a_place = {k: partner(k, True) for k in (1, 2, 4)}
    b_place = {k: partner(k, False) for k in (1, 2, 4)}
    barrier = pltpu.get_barrier_semaphore()

    def tell(sem, blk, chip):
        pl.semaphore_signal(sem, inc=1, device_id=(blk, chip), device_id_type=MESH)

    tell(barrier, other, dp)
    for k in (1, 2, 4):
        tell(barrier, core, number(b_place[k]))
        tell(barrier, core, number(a_place[k]))

    pltpu.make_async_copy(q_hbm, given.at[0], in_sem).start()
    pltpu.make_async_copy(v_hbm, given.at[1], in_sem).start()

    a_chip = [(number(partner(k, True)), rank(partner(k, True), True)) for k in range(8)]
    b_chip = [number(partner(k, False)) for k in range(8)]
    c_me = a_chip[0][1]
    b_me = rank(place, False)

    b_bits = [high_bit(p) if is_low else low_bit(p) for p, is_low in zip(place, A_LOW)]
    lo = pl.multiple_of(core * ROWS, ROWS)

    def plan(src, dst, ssem, rsem, blk, chip):
        return pltpu.make_async_remote_copy(
            src_ref=src, dst_ref=dst, send_sem=ssem, recv_sem=rsem, device_id=(blk, chip), device_id_type=MESH
        )

    def send(*where):
        plan(*where).start()

    def drain(ref, sem):
        pltpu.make_async_copy(ref, ref, sem).wait()

    drain(given, in_sem)

    def unit_rows(value):
        wide = value.astype(F32)
        length = jnp.sqrt(jnp.sum(wide * wide, axis=1, keepdims=True) + TINY)
        return wide / length, length

    qu, ql = unit_rows(given[0])
    vu, vl = unit_rows(given[1])
    q_hat, v_hat = qu.astype(BF16), vu.astype(BF16)
    q_unit[...] = qu
    v_unit[...] = vu
    lens[0] = ql
    lens[1] = vl
    q_own = qbuf.at[c_me, pl.ds(lo, ROWS)]
    qbuf[c_me, pl.ds(lo, ROWS), :] = q_hat
    vbuf[0] = v_hat
    hits = jnp.sum(q_hat.astype(F32) * v_hat.astype(F32), axis=0, keepdims=True)
    ybuf[core * 8 + c_me] = hits[:, :ROWS] + hits[:, ROWS:]

    pl.semaphore_wait(barrier, 7)
    for d in range(3):
        tell(near_sem.at[0], core, a_chip[1 << d][0])
        tell(near_sem.at[1], core, b_chip[1 << d])

    def gather_q(k):
        send(q_own, q_own, big_send, q_recv.at[WAVE[k]], core, a_chip[k][0])

    def gather_v(k):
        send(vbuf.at[0], vbuf.at[SLOT[k]], big_send, v_recv.at[WAVE[k]], core, b_chip[k])

    send(q_own, q_own, big_send, f_recv.at[0], other, dp)
    for k in (4, 2, 1):
        gather_v(k)
        gather_q(k)
    pl.semaphore_wait(near_sem.at[0], 3)
    tell(far_sem.at[0], core, a_chip[1][0])
    for k in (6, 5, 3):
        gather_q(k)
    pl.semaphore_wait(near_sem.at[1], 3)
    tell(far_sem.at[1], core, b_chip[1])
    for k in (6, 5, 3):
        gather_v(k)
    pl.semaphore_wait(far_sem.at[0], 1)
    gather_q(7)
    pl.semaphore_wait(far_sem.at[1], 1)
    gather_v(7)
    def pass_on(ks):
        drain(vbuf.at[0 : len(ks)], q_recv.at[WAVE[ks[0]]])
        for k in ks:
            theirs = qbuf.at[a_chip[k][1], pl.ds(lo, ROWS)]
            send(theirs, theirs, big_send, f_recv.at[0 if k in NEAR else 1], other, dp)

    def weigh(part, first, last, ks):
        rows = slice(first * ROWS, last * ROWS)
        v_part = vbuf[first:last].reshape((last - first) * ROWS, D)
        for k in ks:
            c = a_chip[k][1]
            logits = lax.dot_general(v_part, qbuf[c], (((1,), (1,)), ((), ())), preferred_element_type=F32)
            e = jnp.exp2(logits * (INV_TEMP * LOG2_E))
            spart[part, c, 0:1, :] = jnp.sum(e, axis=0, keepdims=True)
            t_ref[c, rows, :] = e.astype(BF16)

    pass_on(NEAR[1:])
    drain(vbuf.at[1:4], v_recv.at[0])
    drain(qbuf.at[0:2], f_recv.at[0])
    pass_on(FAR[:3])
    weigh(0, 0, 4, NEAR)
    pass_on(FAR[3:])
    drain(qbuf.at[0:2], f_recv.at[1])
    weigh(0, 0, 4, FAR)
    drain(vbuf.at[4:7], v_recv.at[1])
    weigh(1, 4, 7, range(8))
    drain(vbuf.at[7], v_recv.at[2])
    weigh(2, 7, 8, range(8))
    a_me = core * 8 + c_me
    for c in range(8):
        sbuf[a_me, c : c + 1, :] = spart[0, c, 0:1, :] + spart[1, c, 0:1, :] + spart[2, c, 0:1, :]
    v_all = vbuf[...].reshape(8 * ROWS, D)

    def exchange(ref, ssem, rsem):
        for k in ORDER:
            for blk in (core, other):
                send(ref, ref, ssem, rsem, blk, a_chip[k][0])
        send(ref, ref, ssem, rsem, other, dp)

    exchange(sbuf.at[a_me], s_send, s_recv)
    exchange(ybuf.at[a_me], small_send, y_recv)

    for c in range(8):
        ut = lax.dot_general(v_all, t_ref[c], (((0,), (0,)), ((), ())), preferred_element_type=F32)
        ub[0, c] = ut[:, :ROWS].astype(BF16)
        ub[1, c] = ut[:, ROWS:].astype(BF16)
    send(ub.at[other], ud, big_send, d_recv, other, dp)

    drain(ud, d_recv)
    for c in range(8):
        us[c] = (ub[core, c].astype(F32) + ud[c].astype(F32)).astype(BF16)
    for k in ORDER:
        send(us.at[a_chip[k][1]], ur.at[k], big_send, u_recv, core, a_chip[k][0])

    drain(sbuf.at[0:15], s_recv)
    total = sbuf[0]
    for a in range(1, 16):
        total = total + sbuf[a]
    inverse = 1.0 / total
    scales = [jnp.broadcast_to(inverse[c : c + 1, :], (1, 16, 2 * ROWS)).astype(BF16) for c in range(8)]

    def loss_rows():
        drain(ybuf.at[0:15], y_recv)
        hits = ybuf[0]
        for a in range(1, 16):
            hits = hits + ybuf[a]
        logs = jnp.sum(jnp.log(total), axis=0, keepdims=True)
        xbuf[b_me] = (logs[:, :ROWS] + logs[:, ROWS:]) - hits * INV_TEMP
        for k in ORDER:
            send(xbuf.at[b_me], xbuf.at[b_me], small_send, x_recv, core, b_chip[k])

    def pull(rows, n):
        acc = jnp.zeros((n, D), F32)
        for c in range(8):
            probs = rows(c).reshape(n // 16, 16, 2 * ROWS) * scales[c]
            acc = acc + jnp.dot(probs.reshape(n, 2 * ROWS), qbuf[c], preferred_element_type=F32)
        return acc

    def give(k, part, chip):
        wb[k] = part.astype(BF16)
        send(wb.at[k], wr.at[k], big_send, w_recv, core, chip)

    def keep(part):
        w_own[...] = part

    for n, targets in enumerate(W_ORDER):
        ks, rows, chips = [], [], []
        for b in targets:
            bits = ((b >> 2) & 1, (b >> 1) & 1, b & 1)
            dz, dy, dx = (1 - own if bit else own for bit, own in zip(bits, b_bits))
            k = 4 * dz + 2 * dy + dx
            slot = k - dz * (1 - dy) * (1 - dx) + (1 - dz) * dy * dx
            ks.append(k)
            rows.append(pl.ds(pl.multiple_of(slot * ROWS, ROWS), ROWS))
            chips.append(
                number(
                    [
                        (3 - low_bit(p) if bit else low_bit(p)) if is_low else high_bit(p) * (3 - 2 * bit) + bit
                        for p, bit, is_low in zip(place, bits, A_LOW)
                    ]
                )
            )
        acc = pull(lambda c: jnp.concatenate([t_ref[c, r, :] for r in rows]), len(targets) * ROWS)
        for m, b in enumerate(targets):
            part = acc[m * ROWS : (m + 1) * ROWS]
            pl.when(b_me == b)(functools.partial(keep, part))
            pl.when(b_me != b)(functools.partial(give, ks[m], part, chips[m]))
        if n == 0:
            loss_rows()

    mine = lax.broadcasted_iota(jnp.int32, total.shape, 0) == c_me
    s_row = jnp.sum(jnp.where(mine, total, 0.0), axis=0, keepdims=True)
    s_row = jnp.where(core == 0, s_row[:, :ROWS], s_row[:, ROWS:])

    def slope(pull, unit, length):
        along = jnp.sum(unit * pull, axis=1, keepdims=True)
        return (pull - unit * along) / length

    drain(ur.at[1:8], u_recv)
    u_sum = ub[core, c_me].astype(F32) + ud[c_me].astype(F32)
    for k in range(1, 8):
        u_sum = u_sum + ur[k].astype(F32)
    q_pull = (jnp.transpose(u_sum / s_row) - vbuf[0].astype(F32)) * INV_TEMP
    qs_ref[...] = slope(q_pull, q_unit[...], lens[0])

    drain(xbuf.at[0:7], x_recv)
    x_sum = xbuf[0]
    for b in range(1, 8):
        x_sum = x_sum + xbuf[b]
    hits_ref[...] = x_sum

    drain(t_ref.at[:, 0:704, :], big_send)
    drain(sbuf.at[0:15], s_send)
    drain(ybuf.at[0:22], small_send)

    drain(wr.at[1:8], w_recv)
    w_sum = w_own[...]
    for k in range(1, 8):
        w_sum = w_sum + wr[k].astype(F32)
    v_pull = (w_sum - qbuf[c_me, pl.ds(lo, ROWS), :].astype(F32)) * INV_TEMP
    cs_ref[...] = slope(v_pull, v_unit[...], lens[1])


def write_out(l_ref, q_ref, v_ref, l_out, q_out, v_out, l_own, sem):
    q_copy = pltpu.make_async_copy(q_ref, q_out, sem.at[0])
    v_copy = pltpu.make_async_copy(v_ref, v_out, sem.at[1])
    q_copy.start()
    v_copy.start()
    l_own[0, 0] = jnp.sum(l_ref[...]) / BATCH
    l_copy = pltpu.make_async_copy(l_own, l_out, sem.at[2])
    l_copy.start()
    l_copy.wait()
    q_copy.wait()
    v_copy.wait()


def per_device(queries, items):
    dma = pltpu.SemaphoreType.DMA
    vmem = pltpu.VMEM
    parts = pl.pallas_call(
        kernel,
        out_shape=(vmem((1, ROWS), F32), vmem((ROWS, D), F32), vmem((ROWS, D), F32)),
        in_specs=[pl.BlockSpec(memory_space=pltpu.HBM)] * 2,
        out_specs=(pl.BlockSpec(memory_space=vmem),) * 3,
        scratch_shapes=[
            vmem((2, ROWS, D), BF16),
            vmem((ROWS, D), F32),
            vmem((ROWS, D), F32),
            vmem((2, ROWS, 1), F32),
            vmem((8, 2 * ROWS, D), BF16),
            vmem((8, ROWS, D), BF16),
            vmem((8, 8 * ROWS, 2 * ROWS), BF16),
            vmem((16, 8, 2 * ROWS), F32),
            vmem((3, 8, 8, 2 * ROWS), F32),
            vmem((2, 8, D, ROWS), BF16),
            vmem((8, D, ROWS), BF16),
            vmem((8, D, ROWS), BF16),
            vmem((8, D, ROWS), BF16),
            vmem((8, ROWS, D), BF16),
            vmem((ROWS, D), F32),
            vmem((8, ROWS, D), BF16),
            vmem((8, 1, ROWS), F32),
            vmem((24, 1, ROWS), F32),
            dma,
            dma((3,)),
            dma((2,)),
            dma((3,)),
            dma,
            dma,
            dma,
            dma,
            dma,
            dma,
            dma,
            dma,
            dma,
            pltpu.SemaphoreType.REGULAR((2,)),
            pltpu.SemaphoreType.REGULAR((2,)),
        ],
        compiler_params=pltpu.CompilerParams(collective_id=0, has_side_effects=True),
    )(queries, items)
    loss, q_slope, v_slope = pl.pallas_call(
        write_out,
        out_shape=(
            jax.ShapeDtypeStruct((1, 1), F32),
            jax.ShapeDtypeStruct((ROWS, D), F32),
            jax.ShapeDtypeStruct((ROWS, D), F32),
        ),
        in_specs=[pl.BlockSpec(memory_space=vmem)] * 3,
        out_specs=(
            pl.BlockSpec(memory_space=pltpu.HBM),
            pl.BlockSpec(memory_space=pltpu.HBM),
            pl.BlockSpec(memory_space=pltpu.HBM),
        ),
        scratch_shapes=[pltpu.SMEM((1, 1), F32), dma((3,))],
        compiler_params=pltpu.CompilerParams(vmem_limit_bytes=1024 * 1024),
    )(*(pltpu.with_memory_space_constraint(part, vmem) for part in parts))
    return loss.reshape(()), q_slope, v_slope


def solution(mesh):
    spec = P(("blk", "dp"), None)
    return jax.shard_map(
        per_device, mesh=mesh, in_specs=(spec, spec), out_specs=(P(), spec, spec), check_vma=False
    )
```

```python
import functools

import jax
import jax.numpy as jnp
from jax import lax
from jax.experimental import pallas as pl
from jax.experimental.pallas import tpu as pltpu
from jax.sharding import PartitionSpec as P

MESH = pl.DeviceIdType.MESH
ROWS = 128
D = 256
BATCH = 16384
INV_TEMP = 20.0
LOG2_E = 1.4426950408889634
TINY = 1e-12
F32 = jnp.float32
BF16 = jnp.bfloat16
A_LOW = (True, True, True)
SLOT = (0, 1, 2, 4, 3, 5, 6, 7)
NEAR, FAR = (0, 1, 2, 4), (3, 5, 6, 7)
WAVE = (None, 0, 0, 1, 0, 1, 1, 2)
W_ORDER = ((0,), (1, 2), (4, 3), (5, 6), (7,))
ORDER = (7, 3, 5, 6, 1, 2, 4)


def flip_low(p, d):
    return p + 1 - 2 * (p & 1) if d else p


def flip_high(p, d):
    return 3 - p if d else p


def low_bit(p):
    return ((p + 1) >> 1) & 1


def high_bit(p):
    return p >> 1


def kernel(
    q_hbm,
    v_hbm,
    hits_ref,
    qs_ref,
    cs_ref,
    given,
    q_unit,
    v_unit,
    lens,
    qbuf,
    vbuf,
    t_ref,
    sbuf,
    spart,
    ub,
    ud,
    us,
    ur,
    wb,
    w_own,
    wr,
    xbuf,
    ybuf,
    in_sem,
    q_recv,
    f_recv,
    v_recv,
    big_send,
    small_send,
    s_send,
    s_recv,
    d_recv,
    u_recv,
    w_recv,
    x_recv,
    y_recv,
    near_sem,
    far_sem,
):
    core = lax.axis_index("blk")
    other = 1 - core
    dp = lax.axis_index("dp")
    z, y, x = dp >> 4, (dp >> 2) & 3, dp & 3

    place = (z, y, x)

    def partner(k, low):
        steps = ((k >> 2) & 1, (k >> 1) & 1, k & 1)
        zz, yy, xx = (
            (flip_low if is_low == low else flip_high)(p, d) for p, d, is_low in zip(place, steps, A_LOW)
        )
        return zz, yy, xx

    def rank(place, low):
        bits = [(low_bit if is_low == low else high_bit)(p) for p, is_low in zip(place, A_LOW)]
        return bits[0] * 4 + bits[1] * 2 + bits[2]

    def number(place):
        return place[0] * 16 + place[1] * 4 + place[2]

    a_place = {k: partner(k, True) for k in (1, 2, 4)}
    b_place = {k: partner(k, False) for k in (1, 2, 4)}
    barrier = pltpu.get_barrier_semaphore()

    def tell(sem, blk, chip):
        pl.semaphore_signal(sem, inc=1, device_id=(blk, chip), device_id_type=MESH)

    tell(barrier, other, dp)
    for k in (1, 2, 4):
        tell(barrier, core, number(b_place[k]))
        tell(barrier, core, number(a_place[k]))

    pltpu.make_async_copy(q_hbm, given.at[0], in_sem).start()
    pltpu.make_async_copy(v_hbm, given.at[1], in_sem).start()

    a_chip = [(number(partner(k, True)), rank(partner(k, True), True)) for k in range(8)]
    b_chip = [number(partner(k, False)) for k in range(8)]
    c_me = a_chip[0][1]
    b_me = rank(place, False)

    b_bits = [high_bit(p) if is_low else low_bit(p) for p, is_low in zip(place, A_LOW)]
    lo = pl.multiple_of(core * ROWS, ROWS)

    def plan(src, dst, ssem, rsem, blk, chip):
        return pltpu.make_async_remote_copy(
            src_ref=src, dst_ref=dst, send_sem=ssem, recv_sem=rsem, device_id=(blk, chip), device_id_type=MESH
        )

    def send(*where):
        plan(*where).start()

    def drain(ref, sem):
        pltpu.make_async_copy(ref, ref, sem).wait()

    drain(given, in_sem)

    def unit_rows(value):
        wide = value.astype(F32)
        length = jnp.sqrt(jnp.sum(wide * wide, axis=1, keepdims=True) + TINY)
        return wide / length, length

    qu, ql = unit_rows(given[0])
    vu, vl = unit_rows(given[1])
    q_hat, v_hat = qu.astype(BF16), vu.astype(BF16)
    q_unit[...] = qu
    v_unit[...] = vu
    lens[0] = ql
    lens[1] = vl
    q_own = qbuf.at[c_me, pl.ds(lo, ROWS)]
    qbuf[c_me, pl.ds(lo, ROWS), :] = q_hat
    vbuf[0] = v_hat
    hits = jnp.sum(q_hat.astype(F32) * v_hat.astype(F32), axis=0, keepdims=True)
    ybuf[core * 8 + c_me] = hits[:, :ROWS] + hits[:, ROWS:]

    pl.semaphore_wait(barrier, 7)
    for d in range(3):
        tell(near_sem.at[0], core, a_chip[1 << d][0])
        tell(near_sem.at[1], core, b_chip[1 << d])

    def gather_q(k):
        send(q_own, q_own, big_send, q_recv.at[WAVE[k]], core, a_chip[k][0])

    def gather_v(k):
        send(vbuf.at[0], vbuf.at[SLOT[k]], big_send, v_recv.at[WAVE[k]], core, b_chip[k])

    send(q_own, q_own, big_send, f_recv.at[0], other, dp)
    for k in (4, 2, 1):
        gather_v(k)
        gather_q(k)
    pl.semaphore_wait(near_sem.at[0], 3)
    tell(far_sem.at[0], core, a_chip[4][0])
    for k in (6, 5, 3):
        gather_q(k)
    pl.semaphore_wait(near_sem.at[1], 3)
    tell(far_sem.at[1], core, b_chip[4])
    for k in (6, 5, 3):
        gather_v(k)
    pl.semaphore_wait(far_sem.at[0], 1)
    gather_q(7)
    pl.semaphore_wait(far_sem.at[1], 1)
    gather_v(7)
    def pass_on(ks):
        drain(vbuf.at[0 : len(ks)], q_recv.at[WAVE[ks[0]]])
        for k in ks:
            theirs = qbuf.at[a_chip[k][1], pl.ds(lo, ROWS)]
            send(theirs, theirs, big_send, f_recv.at[0 if k in NEAR else 1], other, dp)

    def weigh(part, first, last, ks):
        rows = slice(first * ROWS, last * ROWS)
        v_part = vbuf[first:last].reshape((last - first) * ROWS, D)
        for k in ks:
            c = a_chip[k][1]
            logits = lax.dot_general(v_part, qbuf[c], (((1,), (1,)), ((), ())), preferred_element_type=F32)
            e = jnp.exp2(logits * (INV_TEMP * LOG2_E))
            spart[part, c, 0:1, :] = jnp.sum(e, axis=0, keepdims=True)
            t_ref[c, rows, :] = e.astype(BF16)

    pass_on(NEAR[1:])
    drain(vbuf.at[1:4], v_recv.at[0])
    drain(qbuf.at[0:2], f_recv.at[0])
    pass_on(FAR[:3])
    weigh(0, 0, 4, NEAR)
    pass_on(FAR[3:])
    drain(qbuf.at[0:2], f_recv.at[1])
    weigh(0, 0, 4, FAR)
    drain(vbuf.at[4:7], v_recv.at[1])
    weigh(1, 4, 7, range(8))
    drain(vbuf.at[7], v_recv.at[2])
    weigh(2, 7, 8, range(8))
    a_me = core * 8 + c_me
    for c in range(8):
        sbuf[a_me, c : c + 1, :] = spart[0, c, 0:1, :] + spart[1, c, 0:1, :] + spart[2, c, 0:1, :]
    v_all = vbuf[...].reshape(8 * ROWS, D)

    def exchange(ref, ssem, rsem):
        for k in ORDER:
            for blk in (core, other):
                send(ref, ref, ssem, rsem, blk, a_chip[k][0])
        send(ref, ref, ssem, rsem, other, dp)

    exchange(sbuf.at[a_me], s_send, s_recv)
    exchange(ybuf.at[a_me], small_send, y_recv)

    for c in range(8):
        ut = lax.dot_general(v_all, t_ref[c], (((0,), (0,)), ((), ())), preferred_element_type=F32)
        ub[0, c] = ut[:, :ROWS].astype(BF16)
        ub[1, c] = ut[:, ROWS:].astype(BF16)
    send(ub.at[other], ud, big_send, d_recv, other, dp)

    drain(ud, d_recv)
    for c in range(8):
        us[c] = (ub[core, c].astype(F32) + ud[c].astype(F32)).astype(BF16)
    for k in ORDER:
        send(us.at[a_chip[k][1]], ur.at[k], big_send, u_recv, core, a_chip[k][0])

    drain(sbuf.at[0:15], s_recv)
    total = sbuf[0]
    for a in range(1, 16):
        total = total + sbuf[a]
    inverse = 1.0 / total
    scales = [jnp.broadcast_to(inverse[c : c + 1, :], (1, 16, 2 * ROWS)).astype(BF16) for c in range(8)]

    def loss_rows():
        drain(ybuf.at[0:15], y_recv)
        hits = ybuf[0]
        for a in range(1, 16):
            hits = hits + ybuf[a]
        logs = jnp.sum(jnp.log(total), axis=0, keepdims=True)
        xbuf[b_me] = (logs[:, :ROWS] + logs[:, ROWS:]) - hits * INV_TEMP
        for k in ORDER:
            send(xbuf.at[b_me], xbuf.at[b_me], small_send, x_recv, core, b_chip[k])

    def pull(rows, n):
        acc = jnp.zeros((n, D), F32)
        for c in range(8):
            probs = rows(c).reshape(n // 16, 16, 2 * ROWS) * scales[c]
            acc = acc + jnp.dot(probs.reshape(n, 2 * ROWS), qbuf[c], preferred_element_type=F32)
        return acc

    def give(k, part, chip):
        wb[k] = part.astype(BF16)
        send(wb.at[k], wr.at[k], big_send, w_recv, core, chip)

    def keep(part):
        w_own[...] = part

    for n, targets in enumerate(W_ORDER):
        ks, rows, chips = [], [], []
        for b in targets:
            bits = ((b >> 2) & 1, (b >> 1) & 1, b & 1)
            dz, dy, dx = (1 - own if bit else own for bit, own in zip(bits, b_bits))
            k = 4 * dz + 2 * dy + dx
            slot = k - dz * (1 - dy) * (1 - dx) + (1 - dz) * dy * dx
            ks.append(k)
            rows.append(pl.ds(pl.multiple_of(slot * ROWS, ROWS), ROWS))
            chips.append(
                number(
                    [
                        (3 - low_bit(p) if bit else low_bit(p)) if is_low else high_bit(p) * (3 - 2 * bit) + bit
                        for p, bit, is_low in zip(place, bits, A_LOW)
                    ]
                )
            )
        acc = pull(lambda c: jnp.concatenate([t_ref[c, r, :] for r in rows]), len(targets) * ROWS)
        for m, b in enumerate(targets):
            part = acc[m * ROWS : (m + 1) * ROWS]
            pl.when(b_me == b)(functools.partial(keep, part))
            pl.when(b_me != b)(functools.partial(give, ks[m], part, chips[m]))
        if n == 0:
            loss_rows()

    mine = lax.broadcasted_iota(jnp.int32, total.shape, 0) == c_me
    s_row = jnp.sum(jnp.where(mine, total, 0.0), axis=0, keepdims=True)
    s_row = jnp.where(core == 0, s_row[:, :ROWS], s_row[:, ROWS:])

    def slope(pull, unit, length):
        along = jnp.sum(unit * pull, axis=1, keepdims=True)
        return (pull - unit * along) / length

    drain(ur.at[1:8], u_recv)
    u_sum = ub[core, c_me].astype(F32) + ud[c_me].astype(F32)
    for k in range(1, 8):
        u_sum = u_sum + ur[k].astype(F32)
    q_pull = (jnp.transpose(u_sum / s_row) - vbuf[0].astype(F32)) * INV_TEMP
    qs_ref[...] = slope(q_pull, q_unit[...], lens[0])

    drain(xbuf.at[0:7], x_recv)
    x_sum = xbuf[0]
    for b in range(1, 8):
        x_sum = x_sum + xbuf[b]
    hits_ref[...] = x_sum

    drain(t_ref.at[:, 0:704, :], big_send)
    drain(sbuf.at[0:15], s_send)
    drain(ybuf.at[0:22], small_send)

    drain(wr.at[1:8], w_recv)
    w_sum = w_own[...]
    for k in range(1, 8):
        w_sum = w_sum + wr[k].astype(F32)
    v_pull = (w_sum - qbuf[c_me, pl.ds(lo, ROWS), :].astype(F32)) * INV_TEMP
    cs_ref[...] = slope(v_pull, v_unit[...], lens[1])


def write_out(l_ref, q_ref, v_ref, l_out, q_out, v_out, l_own, sem):
    q_copy = pltpu.make_async_copy(q_ref, q_out, sem.at[0])
    v_copy = pltpu.make_async_copy(v_ref, v_out, sem.at[1])
    q_copy.start()
    v_copy.start()
    l_own[0, 0] = jnp.sum(l_ref[...]) / BATCH
    l_copy = pltpu.make_async_copy(l_own, l_out, sem.at[2])
    l_copy.start()
    q_copy.wait()
    v_copy.wait()
    l_copy.wait()


def per_device(queries, items):
    dma = pltpu.SemaphoreType.DMA
    vmem = pltpu.VMEM
    parts = pl.pallas_call(
        kernel,
        out_shape=(vmem((1, ROWS), F32), vmem((ROWS, D), F32), vmem((ROWS, D), F32)),
        in_specs=[pl.BlockSpec(memory_space=pltpu.HBM)] * 2,
        out_specs=(pl.BlockSpec(memory_space=vmem),) * 3,
        scratch_shapes=[
            vmem((2, ROWS, D), BF16),
            vmem((ROWS, D), F32),
            vmem((ROWS, D), F32),
            vmem((2, ROWS, 1), F32),
            vmem((8, 2 * ROWS, D), BF16),
            vmem((8, ROWS, D), BF16),
            vmem((8, 8 * ROWS, 2 * ROWS), BF16),
            vmem((16, 8, 2 * ROWS), F32),
            vmem((3, 8, 8, 2 * ROWS), F32),
            vmem((2, 8, D, ROWS), BF16),
            vmem((8, D, ROWS), BF16),
            vmem((8, D, ROWS), BF16),
            vmem((8, D, ROWS), BF16),
            vmem((8, ROWS, D), BF16),
            vmem((ROWS, D), F32),
            vmem((8, ROWS, D), BF16),
            vmem((8, 1, ROWS), F32),
            vmem((24, 1, ROWS), F32),
            dma,
            dma((3,)),
            dma((2,)),
            dma((3,)),
            dma,
            dma,
            dma,
            dma,
            dma,
            dma,
            dma,
            dma,
            dma,
            pltpu.SemaphoreType.REGULAR((2,)),
            pltpu.SemaphoreType.REGULAR((2,)),
        ],
        compiler_params=pltpu.CompilerParams(collective_id=0, has_side_effects=True),
    )(queries, items)
    loss, q_slope, v_slope = pl.pallas_call(
        write_out,
        out_shape=(
            jax.ShapeDtypeStruct((1, 1), F32),
            jax.ShapeDtypeStruct((ROWS, D), F32),
            jax.ShapeDtypeStruct((ROWS, D), F32),
        ),
        in_specs=[pl.BlockSpec(memory_space=vmem)] * 3,
        out_specs=(
            pl.BlockSpec(memory_space=pltpu.HBM),
            pl.BlockSpec(memory_space=pltpu.HBM),
            pl.BlockSpec(memory_space=pltpu.HBM),
        ),
        scratch_shapes=[pltpu.SMEM((1, 1), F32), dma((3,))],
        compiler_params=pltpu.CompilerParams(vmem_limit_bytes=1024 * 1024),
    )(*(pltpu.with_memory_space_constraint(part, vmem) for part in parts))
    return loss.reshape(()), q_slope, v_slope


def solution(mesh):
    spec = P(("blk", "dp"), None)
    return jax.shard_map(
        per_device, mesh=mesh, in_specs=(spec, spec), out_specs=(P(), spec, spec), check_vma=False
    )
```

```python
import functools

import jax
import jax.numpy as jnp
from jax import lax
from jax.experimental import pallas as pl
from jax.experimental.pallas import tpu as pltpu
from jax.sharding import PartitionSpec as P

MESH = pl.DeviceIdType.MESH
ROWS = 128
D = 256
BATCH = 16384
INV_TEMP = 20.0
LOG2_E = 1.4426950408889634
TINY = 1e-12
F32 = jnp.float32
BF16 = jnp.bfloat16
A_LOW = (True, True, True)
SLOT = (0, 1, 2, 4, 3, 5, 6, 7)
NEAR, FAR = (0, 1, 2, 4), (3, 5, 6, 7)
WAVE = (None, 0, 0, 1, 0, 1, 1, 2)
W_ORDER = ((0,), (1, 2), (4, 3), (5, 6), (7,))
ORDER = (7, 3, 5, 6, 1, 2, 4)


def flip_low(p, d):
    return p + 1 - 2 * (p & 1) if d else p


def flip_high(p, d):
    return 3 - p if d else p


def low_bit(p):
    return ((p + 1) >> 1) & 1


def high_bit(p):
    return p >> 1


def kernel(
    q_hbm,
    v_hbm,
    hits_ref,
    qs_ref,
    cs_ref,
    given,
    q_unit,
    v_unit,
    lens,
    qbuf,
    vbuf,
    t_ref,
    sbuf,
    spart,
    ub,
    ud,
    us,
    ur,
    wb,
    w_own,
    wr,
    xbuf,
    ybuf,
    in_sem,
    q_recv,
    f_recv,
    v_recv,
    big_send,
    small_send,
    s_send,
    s_recv,
    d_recv,
    u_recv,
    w_recv,
    x_recv,
    y_recv,
    near_sem,
    far_sem,
):
    core = lax.axis_index("blk")
    other = 1 - core
    dp = lax.axis_index("dp")
    z, y, x = dp >> 4, (dp >> 2) & 3, dp & 3

    place = (z, y, x)

    def partner(k, low):
        steps = ((k >> 2) & 1, (k >> 1) & 1, k & 1)
        zz, yy, xx = (
            (flip_low if is_low == low else flip_high)(p, d) for p, d, is_low in zip(place, steps, A_LOW)
        )
        return zz, yy, xx

    def rank(place, low):
        bits = [(low_bit if is_low == low else high_bit)(p) for p, is_low in zip(place, A_LOW)]
        return bits[0] * 4 + bits[1] * 2 + bits[2]

    def number(place):
        return place[0] * 16 + place[1] * 4 + place[2]

    a_place = {k: partner(k, True) for k in (1, 2, 4)}
    b_place = {k: partner(k, False) for k in (1, 2, 4)}
    barrier = pltpu.get_barrier_semaphore()

    def tell(sem, blk, chip):
        pl.semaphore_signal(sem, inc=1, device_id=(blk, chip), device_id_type=MESH)

    tell(barrier, other, dp)
    for k in (1, 2, 4):
        tell(barrier, core, number(b_place[k]))
        tell(barrier, core, number(a_place[k]))

    pltpu.make_async_copy(q_hbm, given.at[0], in_sem).start()
    pltpu.make_async_copy(v_hbm, given.at[1], in_sem).start()

    a_chip = [(number(partner(k, True)), rank(partner(k, True), True)) for k in range(8)]
    b_chip = [number(partner(k, False)) for k in range(8)]
    c_me = a_chip[0][1]
    b_me = rank(place, False)

    b_bits = [high_bit(p) if is_low else low_bit(p) for p, is_low in zip(place, A_LOW)]
    lo = pl.multiple_of(core * ROWS, ROWS)

    def plan(src, dst, ssem, rsem, blk, chip):
        return pltpu.make_async_remote_copy(
            src_ref=src, dst_ref=dst, send_sem=ssem, recv_sem=rsem, device_id=(blk, chip), device_id_type=MESH
        )

    def send(*where):
        plan(*where).start()

    def drain(ref, sem):
        pltpu.make_async_copy(ref, ref, sem).wait()

    drain(given, in_sem)

    def unit_rows(value):
        wide = value.astype(F32)
        length = jnp.sqrt(jnp.sum(wide * wide, axis=1, keepdims=True) + TINY)
        return wide / length, length

    qu, ql = unit_rows(given[0])
    vu, vl = unit_rows(given[1])
    q_hat, v_hat = qu.astype(BF16), vu.astype(BF16)
    q_unit[...] = qu
    v_unit[...] = vu
    lens[0] = ql
    lens[1] = vl
    q_own = qbuf.at[c_me, pl.ds(lo, ROWS)]
    qbuf[c_me, pl.ds(lo, ROWS), :] = q_hat
    vbuf[0] = v_hat
    hits = jnp.sum(q_hat.astype(F32) * v_hat.astype(F32), axis=0, keepdims=True)
    ybuf[core * 8 + c_me] = hits[:, :ROWS] + hits[:, ROWS:]

    pl.semaphore_wait(barrier, 7)
    for d in range(3):
        tell(near_sem.at[0], core, a_chip[1 << d][0])
        tell(near_sem.at[1], core, b_chip[1 << d])

    def gather_q(k):
        send(q_own, q_own, big_send, q_recv.at[WAVE[k]], core, a_chip[k][0])

    def gather_v(k):
        send(vbuf.at[0], vbuf.at[SLOT[k]], big_send, v_recv.at[WAVE[k]], core, b_chip[k])

    send(q_own, q_own, big_send, f_recv.at[0], other, dp)
    for k in (4, 2, 1):
        gather_v(k)
        gather_q(k)
    pl.semaphore_wait(near_sem.at[0], 3)
    tell(far_sem.at[0], core, a_chip[1][0])
    for k in (6, 5, 3):
        gather_q(k)
    pl.semaphore_wait(near_sem.at[1], 3)
    tell(far_sem.at[1], core, b_chip[1])
    for k in (6, 5, 3):
        gather_v(k)
    pl.semaphore_wait(far_sem.at[0], 1)
    gather_q(7)
    pl.semaphore_wait(far_sem.at[1], 1)
    gather_v(7)
    def pass_on(ks):
        drain(vbuf.at[0 : len(ks)], q_recv.at[WAVE[ks[0]]])
        for k in ks:
            theirs = qbuf.at[a_chip[k][1], pl.ds(lo, ROWS)]
            send(theirs, theirs, big_send, f_recv.at[0 if k in NEAR else 1], other, dp)

    def weigh(part, first, last, ks):
        rows = slice(first * ROWS, last * ROWS)
        v_part = vbuf[first:last].reshape((last - first) * ROWS, D)
        for k in ks:
            c = a_chip[k][1]
            logits = lax.dot_general(v_part, qbuf[c], (((1,), (1,)), ((), ())), preferred_element_type=F32)
            e = jnp.exp2(logits * (INV_TEMP * LOG2_E))
            spart[part, c, 0:1, :] = jnp.sum(e, axis=0, keepdims=True)
            t_ref[c, rows, :] = e.astype(BF16)

    pass_on(NEAR[1:])
    drain(vbuf.at[1:4], v_recv.at[0])
    drain(qbuf.at[0:2], f_recv.at[0])
    pass_on(FAR[:3])
    weigh(0, 0, 4, NEAR)
    pass_on(FAR[3:])
    drain(qbuf.at[0:2], f_recv.at[1])
    weigh(0, 0, 4, FAR)
    drain(vbuf.at[4:7], v_recv.at[1])
    weigh(1, 4, 7, range(8))
    drain(vbuf.at[7], v_recv.at[2])
    weigh(2, 7, 8, range(8))
    a_me = core * 8 + c_me
    for c in range(8):
        sbuf[a_me, c : c + 1, :] = spart[0, c, 0:1, :] + spart[1, c, 0:1, :] + spart[2, c, 0:1, :]
    v_all = vbuf[...].reshape(8 * ROWS, D)

    def exchange(ref, ssem, rsem):
        for k in ORDER:
            for blk in (core, other):
                send(ref, ref, ssem, rsem, blk, a_chip[k][0])
        send(ref, ref, ssem, rsem, other, dp)

    exchange(sbuf.at[a_me], s_send, s_recv)
    exchange(ybuf.at[a_me], small_send, y_recv)

    for c in range(8):
        ut = lax.dot_general(v_all, t_ref[c], (((0,), (0,)), ((), ())), preferred_element_type=F32)
        ub[0, c] = ut[:, :ROWS].astype(BF16)
        ub[1, c] = ut[:, ROWS:].astype(BF16)
    send(ub.at[other], ud, big_send, d_recv, other, dp)

    drain(ud, d_recv)
    for c in range(8):
        us[c] = (ub[core, c].astype(F32) + ud[c].astype(F32)).astype(BF16)
    for k in ORDER:
        send(us.at[a_chip[k][1]], ur.at[k], big_send, u_recv, core, a_chip[k][0])

    drain(sbuf.at[0:15], s_recv)
    total = sbuf[0]
    for a in range(1, 16):
        total = total + sbuf[a]
    inverse = 1.0 / total
    scales = [jnp.broadcast_to(inverse[c : c + 1, :], (1, 16, 2 * ROWS)).astype(BF16) for c in range(8)]

    def loss_rows():
        drain(ybuf.at[0:15], y_recv)
        hits = ybuf[0]
        for a in range(1, 16):
            hits = hits + ybuf[a]
        logs = jnp.sum(jnp.log(total), axis=0, keepdims=True)
        xbuf[b_me] = (logs[:, :ROWS] + logs[:, ROWS:]) - hits * INV_TEMP
        for k in ORDER:
            send(xbuf.at[b_me], xbuf.at[b_me], small_send, x_recv, core, b_chip[k])

    def pull(rows, n):
        acc = jnp.zeros((n, D), F32)
        for c in range(8):
            probs = rows(c).reshape(n // 16, 16, 2 * ROWS) * scales[c]
            acc = acc + jnp.dot(probs.reshape(n, 2 * ROWS), qbuf[c], preferred_element_type=F32)
        return acc

    def give(k, part, chip):
        wb[k] = part.astype(BF16)
        send(wb.at[k], wr.at[k], big_send, w_recv, core, chip)

    def keep(part):
        w_own[...] = part

    for n, targets in enumerate(W_ORDER):
        ks, rows, chips = [], [], []
        for b in targets:
            bits = ((b >> 2) & 1, (b >> 1) & 1, b & 1)
            dz, dy, dx = (1 - own if bit else own for bit, own in zip(bits, b_bits))
            k = 4 * dz + 2 * dy + dx
            slot = k - dz * (1 - dy) * (1 - dx) + (1 - dz) * dy * dx
            ks.append(k)
            rows.append(pl.ds(pl.multiple_of(slot * ROWS, ROWS), ROWS))
            chips.append(
                number(
                    [
                        (3 - low_bit(p) if bit else low_bit(p)) if is_low else high_bit(p) * (3 - 2 * bit) + bit
                        for p, bit, is_low in zip(place, bits, A_LOW)
                    ]
                )
            )
        acc = pull(lambda c: jnp.concatenate([t_ref[c, r, :] for r in rows]), len(targets) * ROWS)
        for m, b in enumerate(targets):
            part = acc[m * ROWS : (m + 1) * ROWS]
            pl.when(b_me == b)(functools.partial(keep, part))
            pl.when(b_me != b)(functools.partial(give, ks[m], part, chips[m]))
        if n == 1:
            loss_rows()

    mine = lax.broadcasted_iota(jnp.int32, total.shape, 0) == c_me
    s_row = jnp.sum(jnp.where(mine, total, 0.0), axis=0, keepdims=True)
    s_row = jnp.where(core == 0, s_row[:, :ROWS], s_row[:, ROWS:])

    def slope(pull, unit, length):
        along = jnp.sum(unit * pull, axis=1, keepdims=True)
        return (pull - unit * along) / length

    drain(ur.at[1:8], u_recv)
    u_sum = ub[core, c_me].astype(F32) + ud[c_me].astype(F32)
    for k in range(1, 8):
        u_sum = u_sum + ur[k].astype(F32)
    q_pull = (jnp.transpose(u_sum / s_row) - vbuf[0].astype(F32)) * INV_TEMP
    qs_ref[...] = slope(q_pull, q_unit[...], lens[0])

    drain(xbuf.at[0:7], x_recv)
    x_sum = xbuf[0]
    for b in range(1, 8):
        x_sum = x_sum + xbuf[b]
    hits_ref[...] = x_sum

    drain(t_ref.at[:, 0:704, :], big_send)
    drain(sbuf.at[0:15], s_send)
    drain(ybuf.at[0:22], small_send)

    drain(wr.at[1:8], w_recv)
    w_sum = w_own[...]
    for k in range(1, 8):
        w_sum = w_sum + wr[k].astype(F32)
    v_pull = (w_sum - qbuf[c_me, pl.ds(lo, ROWS), :].astype(F32)) * INV_TEMP
    cs_ref[...] = slope(v_pull, v_unit[...], lens[1])


def write_out(l_ref, q_ref, v_ref, l_out, q_out, v_out, l_own, sem):
    q_copy = pltpu.make_async_copy(q_ref, q_out, sem.at[0])
    v_copy = pltpu.make_async_copy(v_ref, v_out, sem.at[1])
    q_copy.start()
    v_copy.start()
    l_own[0, 0] = jnp.sum(l_ref[...]) / BATCH
    l_copy = pltpu.make_async_copy(l_own, l_out, sem.at[2])
    l_copy.start()
    l_copy.wait()
    q_copy.wait()
    v_copy.wait()


def per_device(queries, items):
    dma = pltpu.SemaphoreType.DMA
    vmem = pltpu.VMEM
    parts = pl.pallas_call(
        kernel,
        out_shape=(vmem((1, ROWS), F32), vmem((ROWS, D), F32), vmem((ROWS, D), F32)),
        in_specs=[pl.BlockSpec(memory_space=pltpu.HBM)] * 2,
        out_specs=(pl.BlockSpec(memory_space=vmem),) * 3,
        scratch_shapes=[
            vmem((2, ROWS, D), BF16),
            vmem((ROWS, D), F32),
            vmem((ROWS, D), F32),
            vmem((2, ROWS, 1), F32),
            vmem((8, 2 * ROWS, D), BF16),
            vmem((8, ROWS, D), BF16),
            vmem((8, 8 * ROWS, 2 * ROWS), BF16),
            vmem((16, 8, 2 * ROWS), F32),
            vmem((3, 8, 8, 2 * ROWS), F32),
            vmem((2, 8, D, ROWS), BF16),
            vmem((8, D, ROWS), BF16),
            vmem((8, D, ROWS), BF16),
            vmem((8, D, ROWS), BF16),
            vmem((8, ROWS, D), BF16),
            vmem((ROWS, D), F32),
            vmem((8, ROWS, D), BF16),
            vmem((8, 1, ROWS), F32),
            vmem((24, 1, ROWS), F32),
            dma,
            dma((3,)),
            dma((2,)),
            dma((3,)),
            dma,
            dma,
            dma,
            dma,
            dma,
            dma,
            dma,
            dma,
            dma,
            pltpu.SemaphoreType.REGULAR((2,)),
            pltpu.SemaphoreType.REGULAR((2,)),
        ],
        compiler_params=pltpu.CompilerParams(collective_id=0, has_side_effects=True),
    )(queries, items)
    loss, q_slope, v_slope = pl.pallas_call(
        write_out,
        out_shape=(
            jax.ShapeDtypeStruct((1, 1), F32),
            jax.ShapeDtypeStruct((ROWS, D), F32),
            jax.ShapeDtypeStruct((ROWS, D), F32),
        ),
        in_specs=[pl.BlockSpec(memory_space=vmem)] * 3,
        out_specs=(
            pl.BlockSpec(memory_space=pltpu.HBM),
            pl.BlockSpec(memory_space=pltpu.HBM),
            pl.BlockSpec(memory_space=pltpu.HBM),
        ),
        scratch_shapes=[pltpu.SMEM((1, 1), F32), dma((3,))],
        compiler_params=pltpu.CompilerParams(vmem_limit_bytes=1024 * 1024),
    )(*(pltpu.with_memory_space_constraint(part, vmem) for part in parts))
    return loss.reshape(()), q_slope, v_slope


def solution(mesh):
    spec = P(("blk", "dp"), None)
    return jax.shard_map(
        per_device, mesh=mesh, in_specs=(spec, spec), out_specs=(P(), spec, spec), check_vma=False
    )
```
